256 devices in a mesh: trial: 4 (over x_lo, core), north: 16 (over z_hi, y, x_hi), east: 4 (over z_lo).
Axes of the slice: x: 4 (x_hi: 2, x_lo: 2; x = x_hi * 2 + x_lo), y: 4, z: 8 (z_hi: 2, z_lo: 4; z = z_hi * 4 + z_lo), core: 2. Of those that a mesh axis runs over, the one named last changes fastest.
Arguments:
- pair_state: bfloat16 [1536, 384, 128], P(('trial', 'north'), 'east'), parts along dimension 0, may hold values from -6 to 6
- in_gain: float32 [128], replicated, may hold values from 0.25 to 1.75
- left_weight: bfloat16 [512, 128], P('trial'), parts along dimension 0, may hold values from -0.5 to 0.5
- right_weight: bfloat16 [512, 128], P('trial'), parts along dimension 0, may hold values from -0.5 to 0.5
- left_gate: bfloat16 [512, 128], P('trial'), parts along dimension 0, may hold values from -0.5 to 0.5
- right_gate: bfloat16 [512, 128], P('trial'), parts along dimension 0, may hold values from -0.5 to 0.5
- mid_gain: float32 [128], replicated, may hold values from 0.25 to 1.75
- out_weight: bfloat16 [512, 128], P('trial'), parts along dimension 0, may hold values from -0.5 to 0.5
- out_gate: bfloat16 [512, 128], P('trial'), parts along dimension 0, may hold values from -0.5 to 0.5
Outputs:
- triangle_out: bfloat16 [1536, 384, 128], P(('trial', 'north'), 'east'), parts along dimension 0
The draws below stay inside these ranges and needn't reach their ends.
There are 4 independent parts, one for each index of `trial`. The reference program is written for one: setup_inputs(seed, part) draws one part's arguments, and reference() takes and returns one part's arrays. A program takes and returns all parts, laid end to end along the dimension named above; an argument that names none is the same for every part. Nothing has to cross between parts.
All inputs are finite; a program needn't handle non-finite values.
Results may differ from the reference program's by a relative error of at most 0.015.
Values may be sent and summed in bfloat16 or wider, within the bound.
A program may use at most 64 MiB of HBM per device.

```python
import jax
import jax.numpy as jnp
from jax import lax

RESIDUES = 384
PAIR_WIDTH = 128
MIX_WIDTH = 128


def block_scale(own_key, shape, pieces, low, top_value):
    def one(axis_at, blocks):
        draws = jax.random.uniform(jax.random.fold_in(jax.random.fold_in(own_key, 6), axis_at), (blocks,), jnp.float32, low / len(pieces), top_value / len(pieces))
        return jnp.repeat(jnp.exp(draws), shape[axis_at] // blocks).reshape((-1,) + (1,) * (len(shape) - axis_at - 1))

    level = one(*pieces[0])
    for cut in pieces[1:]:
        level = level * one(*cut)
    return level


def scatter_about(stream_key, shape, spread, reach, shards=(), kind=jnp.bfloat16):
    values = spread * jax.random.normal(stream_key, shape, jnp.float32)
    if shards:
        values = values * block_scale(stream_key, shape, shards, -0.22, 0.18)
    return jnp.clip(values, -reach, reach).astype(kind)


def setup_inputs(seed: int = 0, part: int = 0) -> dict:
    keys = jax.random.split(jax.random.key(seed), 10)
    own_keys = jax.random.split(jax.random.fold_in(keys[9], part), 10)
    pair_state = scatter_about(own_keys[0], (RESIDUES, RESIDUES, PAIR_WIDTH), 1.0, 6.0, ((0, 16), (1, 4)))
    in_gain = jnp.clip(1.0 + 0.15 * jax.random.normal(keys[1], (PAIR_WIDTH,), jnp.float32), 0.25, 1.75)
    left_weight = scatter_about(own_keys[2], (PAIR_WIDTH, MIX_WIDTH), PAIR_WIDTH ** -0.5, 0.5)
    right_weight = scatter_about(own_keys[3], (PAIR_WIDTH, MIX_WIDTH), PAIR_WIDTH ** -0.5, 0.5)
    left_gate = scatter_about(own_keys[4], (PAIR_WIDTH, MIX_WIDTH), PAIR_WIDTH ** -0.5, 0.5)
    right_gate = scatter_about(own_keys[5], (PAIR_WIDTH, MIX_WIDTH), PAIR_WIDTH ** -0.5, 0.5)
    mid_gain = jnp.clip(1.0 + 0.15 * jax.random.normal(keys[6], (MIX_WIDTH,), jnp.float32), 0.25, 1.75)
    out_weight = scatter_about(own_keys[7], (MIX_WIDTH, PAIR_WIDTH), MIX_WIDTH ** -0.5, 0.5)
    out_gate = scatter_about(own_keys[8], (PAIR_WIDTH, PAIR_WIDTH), PAIR_WIDTH ** -0.5, 0.5)
    return {"pair_state": pair_state, "in_gain": in_gain, "left_weight": left_weight, "right_weight": right_weight, "left_gate": left_gate, "right_gate": right_gate, "mid_gain": mid_gain, "out_weight": out_weight, "out_gate": out_gate}


def norm_channels(values, channel_gain):
    centred = values - lax.optimization_barrier(jnp.mean(values, axis=-1, keepdims=True))
    return centred * lax.rsqrt(lax.optimization_barrier(jnp.mean(centred * centred, axis=-1, keepdims=True)) + 1e-05) * channel_gain

def make_factors(pair_in, in_gain, left_weight, right_weight, left_gate, right_gate):
    ready = norm_channels(pair_in.astype(jnp.float32), in_gain).astype(jnp.bfloat16)
    ready = lax.optimization_barrier(ready)
    left = jnp.einsum('ijc,cd->ijd', ready.astype(jnp.float32), left_weight.astype(jnp.float32))
    left = left * jax.nn.sigmoid(jnp.einsum('ijc,cd->ijd', ready.astype(jnp.float32), left_gate.astype(jnp.float32)))
    right = jnp.einsum('ijc,cd->ijd', ready.astype(jnp.float32), right_weight.astype(jnp.float32))
    right = right * jax.nn.sigmoid(jnp.einsum('ijc,cd->ijd', ready.astype(jnp.float32), right_gate.astype(jnp.float32)))
    return (ready, left.astype(jnp.bfloat16), right.astype(jnp.bfloat16))

def to_pair(mixed, ready, mid_gain, out_weight, out_gate):
    scaled = norm_channels(mixed.astype(jnp.float32), mid_gain).astype(jnp.bfloat16)
    scaled = lax.optimization_barrier(scaled)
    gate = jax.nn.sigmoid(jnp.einsum('ijc,cd->ijd', ready.astype(jnp.float32), out_gate.astype(jnp.float32)))
    return (jnp.einsum('ijd,dc->ijc', scaled.astype(jnp.float32), out_weight.astype(jnp.float32)) * gate).astype(jnp.bfloat16)

def reference(pair_state, in_gain, left_weight, right_weight, left_gate, right_gate, mid_gain, out_weight, out_gate):
    ready, left, right = make_factors(pair_state, in_gain, left_weight, right_weight, left_gate, right_gate)
    left, right = lax.optimization_barrier((left, right))

    def one_channel(pair_of):
        return (jnp.dot(pair_of[0], pair_of[1].T, preferred_element_type=jnp.float32) * RESIDUES ** (-0.5)).astype(jnp.bfloat16)
    mixed = jnp.moveaxis(lax.map(one_channel, (jnp.moveaxis(left, -1, 0), jnp.moveaxis(right, -1, 0))), 0, -1)
    mixed = lax.optimization_barrier(mixed)
    return to_pair(mixed, ready, mid_gain, out_weight, out_gate)
```

```python
import functools

import jax
import jax.numpy as jnp
from jax import lax
from jax.experimental import pallas as pl
from jax.experimental.pallas import tpu as pltpu
from jax.sharding import PartitionSpec as P

MESH = pl.DeviceIdType.MESH


def norm_channels(values, channel_gain, axis=-1):
    centred = values - jnp.mean(values, axis=axis, keepdims=True)
    return (
        centred
        * lax.rsqrt(jnp.mean(centred * centred, axis=axis, keepdims=True) + 1e-05)
        * channel_gain
    )


def exchange_kernel(north, east, src, dst, send_sem, recv_sem, own_sem):
    n = lax.axis_index("north")
    e = lax.axis_index("east")
    count = north * east
    me = n * east + e

    def peer(k):
        q = lax.rem(me + k, count)
        return q, {"north": q // east, "east": lax.rem(q, east)}

    barrier = pltpu.get_barrier_semaphore()

    def greet(k, carry):
        pl.semaphore_signal(barrier, inc=1, device_id=peer(k)[1], device_id_type=MESH)
        return carry

    lax.fori_loop(1, count, greet, 0)
    pl.semaphore_wait(barrier, count - 1)
    own = pltpu.make_async_copy(src.at[me], dst.at[me], own_sem)
    own.start()

    def send(k, carry):
        q, device = peer(k)
        pltpu.make_async_remote_copy(
            src_ref=src.at[q],
            dst_ref=dst.at[me],
            send_sem=send_sem,
            recv_sem=recv_sem,
            device_id=device,
            device_id_type=MESH,
        ).start()
        return carry

    lax.fori_loop(1, count, send, 0)
    own.wait()
    everything = pltpu.make_async_remote_copy(
        src_ref=src.at[pl.ds(0, count - 1)],
        dst_ref=dst.at[pl.ds(0, count - 1)],
        send_sem=send_sem,
        recv_sem=recv_sem,
        device_id={"north": n, "east": e},
        device_id_type=MESH,
    )
    everything.wait_recv()
    everything.wait_send()


def exchange(pieces, north, east, collective_id):
    return pl.pallas_call(
        functools.partial(exchange_kernel, north, east),
        out_shape=jax.ShapeDtypeStruct(pieces.shape, pieces.dtype),
        in_specs=[pl.BlockSpec(memory_space=pltpu.VMEM)],
        out_specs=pl.BlockSpec(memory_space=pltpu.VMEM),
        scratch_shapes=[
            pltpu.SemaphoreType.DMA,
            pltpu.SemaphoreType.DMA,
            pltpu.SemaphoreType.DMA,
        ],
        compiler_params=pltpu.CompilerParams(
            collective_id=collective_id, has_side_effects=True
        ),
    )(pieces)


def local(
    north,
    east,
    pair_state,
    in_gain,
    left_weight,
    right_weight,
    left_gate,
    right_gate,
    mid_gain,
    out_weight,
    out_gate,
):
    rows, cols, width = pair_state.shape
    group = north * east
    mix = left_weight.shape[1]
    own = mix // group
    ready = norm_channels(pair_state.astype(jnp.float32), in_gain).astype(jnp.bfloat16)
    ready = ready.reshape(rows * cols, width)

    def factor(weight, gate):
        value = jnp.einsum("pc,cd->dp", ready, weight, preferred_element_type=jnp.float32)
        value = value * jax.nn.sigmoid(
            jnp.einsum("pc,cd->dp", ready, gate, preferred_element_type=jnp.float32)
        )
        return value.astype(jnp.bfloat16).reshape(group, own, rows * cols)

    left = factor(left_weight, left_gate)
    right = factor(right_weight, right_gate)
    got = exchange(jnp.concatenate([left, right], axis=1), north, east, 0)
    got = got.reshape(north, east, 2, own, rows, cols).transpose(2, 3, 0, 4, 1, 5)
    got = got.reshape(2, own, north * rows, east * cols)
    mixed = jnp.einsum("dik,djk->dij", got[0], got[1], preferred_element_type=jnp.float32)
    mixed = (mixed * (east * cols) ** (-0.5)).astype(jnp.bfloat16)
    mixed = mixed.reshape(own, north, rows, east, cols).transpose(1, 3, 0, 2, 4)
    mixed = exchange(mixed.reshape(group, own, rows * cols), north, east, 1)
    mixed = mixed.reshape(mix, rows * cols)
    scaled = norm_channels(mixed.astype(jnp.float32), mid_gain[:, None], 0).astype(jnp.bfloat16)
    gate = jax.nn.sigmoid(
        jnp.einsum("pc,cd->pd", ready, out_gate, preferred_element_type=jnp.float32)
    )
    out = jnp.einsum("dp,dc->pc", scaled, out_weight, preferred_element_type=jnp.float32)
    return (out * gate).astype(jnp.bfloat16).reshape(rows, cols, width)


def solution(mesh):
    north, east = mesh.shape["north"], mesh.shape["east"]
    return jax.shard_map(
        functools.partial(local, north, east),
        mesh=mesh,
        in_specs=(
            P(("trial", "north"), "east", None),
            P(),
            P("trial", None),
            P("trial", None),
            P("trial", None),
            P("trial", None),
            P(),
            P("trial", None),
            P("trial", None),
        ),
        out_specs=P(("trial", "north"), "east", None),
        check_vma=False,
    )
```

```python
import functools

import jax
import jax.numpy as jnp
from jax import lax
from jax.experimental import pallas as pl
from jax.experimental.pallas import tpu as pltpu
from jax.sharding import PartitionSpec as P

MESH = pl.DeviceIdType.MESH
BF16, F32 = jnp.bfloat16, jnp.float32
EPS = 1e-05


def dot_nt(a, b):
    return lax.dot_general(a, b, (((1,), (1,)), ((), ())), preferred_element_type=F32)


def iota(shape, axis):
    return lax.broadcasted_iota(jnp.int32, shape, axis)


def sigmoid(x):
    return jax.nn.sigmoid(x)


def kernel(
    north,
    east,
    rows,
    cols,
    x_ref,
    in_gain_ref,
    lw_ref,
    rw_ref,
    lg_ref,
    rg_ref,
    mid_gain_ref,
    ow_ref,
    og_ref,
    out_ref,
    ready_ref,
    gate_ref,
    send1,
    recv1,
    left_ref,
    right_ref,
    send2,
    recv2,
    send_sem1,
    recv_sem1,
    send_sem2,
    recv_sem2,
):
    width = x_ref.shape[1]
    group = north * east
    half = rows // 2
    lines = half * cols
    n = lax.axis_index("north")
    e = lax.axis_index("east")
    me = e * north + n

    def device(c, k):
        return lax.rem(e + c, east), lax.rem(n + k, north)

    def each_peer(do):
        for c in range(east):

            def body(k, carry, c=c):
                do(*device(c, k))
                return carry

            lax.fori_loop(1 if c == 0 else 0, north, body, 0)

    barrier = pltpu.get_barrier_semaphore()
    each_peer(
        lambda pe, pn: pl.semaphore_signal(
            barrier, inc=1, device_id={"north": pn, "east": pe}, device_id_type=MESH
        )
    )

    x = x_ref[...].astype(F32)
    centred = x - jnp.mean(x, axis=-1, keepdims=True)
    ready = (
        centred * lax.rsqrt(jnp.mean(centred * centred, axis=-1, keepdims=True) + EPS)
        * in_gain_ref[...]
    ).astype(BF16)
    ready_ref[...] = ready
    both = jnp.concatenate([ready_ref[:lines, :], ready_ref[lines:, :]], axis=1)

    def send_all(src, dst, send_sem, recv_sem):
        dst[me] = src[me]
        each_peer(
            lambda pe, pn: pltpu.make_async_remote_copy(
                src_ref=src.at[pe * north + pn],
                dst_ref=dst.at[me],
                send_sem=send_sem,
                recv_sem=recv_sem,
                device_id={"north": pn, "east": pe},
                device_id_type=MESH,
            ).start()
        )

    def all_of(src, dst, send_sem, recv_sem):
        return pltpu.make_async_remote_copy(
            src_ref=src.at[pl.ds(0, group - 1)],
            dst_ref=dst.at[pl.ds(0, group - 1)],
            send_sem=send_sem,
            recv_sem=recv_sem,
            device_id={"north": n, "east": e},
            device_id_type=MESH,
        )

    r = iota((4 * group, width), 0)
    d = iota((4 * group, width), 1)
    parity = (r & 1) == 0

    def spread(weights, ch):
        picked = 0.0
        for f, w in enumerate(weights):
            pick = (((r >> 1) & 1) == f) & (d == (r >> 2) + ch * group)
            picked = picked + dot_nt(jnp.where(pick, 1.0, 0.0).astype(BF16), w[...])
        return jnp.concatenate(
            [jnp.where(parity, picked, 0.0), jnp.where(parity, 0.0, picked)], axis=1
        ).astype(BF16)

    for ch in range(2):
        value = dot_nt(spread((lw_ref, rw_ref), ch), both)
        gate = dot_nt(spread((lg_ref, rg_ref), ch), both)
        value = (value * sigmoid(gate)).reshape(group, 4, lines)
        send1[ch] = value.astype(BF16)
        if ch == 0:
            pl.semaphore_wait(barrier, group - 1)
        send_all(send1.at[ch], recv1.at[ch], send_sem1.at[ch], recv_sem1.at[ch])

    gate_ref[...] = sigmoid(
        jnp.dot(ready_ref[...], og_ref[...], preferred_element_type=F32)
    )
    left_ref[...] = jnp.zeros_like(left_ref)
    right_ref[...] = jnp.zeros_like(right_ref)

    per = north // east * 2
    for ch in range(2):
        all_of(send1.at[ch], recv1.at[ch], send_sem1.at[ch], recv_sem1.at[ch]).wait_recv()
        for s in range(east):
            lines_l = recv1[ch, north * s : north * (s + 1), 0:2, :].reshape(2 * north, lines)
            lines_r = recv1[ch, north * s : north * (s + 1), 2:4, :].reshape(2 * north, lines)
            for i in range(half):
                left_ref[2 * north * i : 2 * north * (i + 1), 128 * s : 128 * s + cols] = (
                    lines_l[:, cols * i : cols * (i + 1)]
                )
                piece = lines_r[:, cols * i : cols * (i + 1)]
                for t in range(east):
                    right_ref[128 * t + per * i : 128 * t + per * (i + 1), 128 * s : 128 * s + cols] = (
                        piece[per * t : per * (t + 1)]
                    )
        mixed = dot_nt(left_ref[...], right_ref[...]) * (cols * east) ** (-0.5)
        for t in range(east):
            strip = jnp.concatenate(
                [
                    mixed[2 * north * i : 2 * north * (i + 1), 128 * t : 128 * t + cols]
                    for i in range(half)
                ],
                axis=1,
            )
            send2[ch, north * t : north * (t + 1)] = strip.reshape(north, 2, lines).astype(BF16)
        send_all(send2.at[ch], recv2.at[ch], send_sem2.at[ch], recv_sem2.at[ch])

    mid_gain = jnp.broadcast_to(mid_gain_ref[...], (width, width)).T
    mid_gain = jnp.broadcast_to(mid_gain[:, None, :], (width, 2, width)).reshape(2 * width, width)
    mid_gain = jnp.concatenate([mid_gain] * 3, axis=1)
    weight = ow_ref[...].astype(F32)
    weight = jnp.broadcast_to(weight[:, None, :], (width, 2, width)).reshape(2 * width, width)
    first = (iota((2 * width, width), 0) & 1) == 0
    weight = jnp.concatenate(
        [jnp.where(first, weight, 0.0), jnp.where(first, 0.0, weight)], axis=1
    ).astype(BF16)
    tile = 4 * cols
    lane = iota((tile, tile), 1)
    block = jnp.where(lane >= 2 * cols, 2, 0)
    block = block + jnp.where(lane - block * cols >= cols, 1, 0)
    rest = lane - block * cols
    target = block * cols + ((rest & (per - 1)) >> 1) * rows + (rest & 1) * half + (rest >> 3)
    order = jnp.where(iota((tile, tile), 0) == target, 1.0, 0.0).astype(BF16)

    for ch in range(2):
        all_of(send2.at[ch], recv2.at[ch], send_sem2.at[ch], recv_sem2.at[ch]).wait_recv()

    def fold(total):
        total = jnp.sum(total.reshape(2 * width // 8, 8, tile), axis=0)
        total = total + pltpu.roll(total, 4, 0)
        total = total + pltpu.roll(total, 2, 0)
        return (total * (1.0 / width))[None]

    for g in range(lines // tile):
        lanes = slice(g * tile, (g + 1) * tile)
        mixed = recv2[:, :, :, lanes].reshape(2 * width, tile).astype(F32)
        centred = mixed.reshape(2 * width // 8, 8, tile) - fold(mixed)
        scale = lax.rsqrt(fold((centred * centred).reshape(2 * width, tile)) + EPS)
        scaled = ((centred * scale).reshape(2 * width, tile) * mid_gain).astype(BF16)
        turned = dot_nt(order, scaled).astype(BF16)
        result = jnp.dot(turned, weight, preferred_element_type=F32)
        for h in range(2):
            at = slice(h * lines + g * tile, h * lines + (g + 1) * tile)
            out_ref[at, :] = (
                result[:, h * width : (h + 1) * width] * gate_ref[at, :]
            ).astype(BF16)

    for ch in range(2):
        for src, dst, a, b in (
            (send1, recv1, send_sem1, recv_sem1),
            (send2, recv2, send_sem2, recv_sem2),
        ):
            all_of(src.at[ch], dst.at[ch], a.at[ch], b.at[ch]).wait_send()


def local(
    north,
    east,
    pair_state,
    in_gain,
    left_weight,
    right_weight,
    left_gate,
    right_gate,
    mid_gain,
    out_weight,
    out_gate,
):
    rows, cols, width = pair_state.shape
    lines = rows // 2 * cols
    group = north * east
    vmem = pl.BlockSpec(memory_space=pltpu.VMEM)
    out = pl.pallas_call(
        functools.partial(kernel, north, east, rows, cols),
        out_shape=jax.ShapeDtypeStruct((rows * cols, width), BF16),
        in_specs=[vmem] * 9,
        out_specs=vmem,
        scratch_shapes=[
            pltpu.VMEM((rows * cols, width), BF16),
            pltpu.VMEM((rows * cols, width), F32),
            pltpu.VMEM((2, group, 4, lines), BF16),
            pltpu.VMEM((2, group, 4, lines), BF16),
            pltpu.VMEM((rows * north, 128 * east), BF16),
            pltpu.VMEM((128 * east, 128 * east), BF16),
            pltpu.VMEM((2, group, 2, lines), BF16),
            pltpu.VMEM((2, group, 2, lines), BF16),
            pltpu.SemaphoreType.DMA((2,)),
            pltpu.SemaphoreType.DMA((2,)),
            pltpu.SemaphoreType.DMA((2,)),
            pltpu.SemaphoreType.DMA((2,)),
        ],
        compiler_params=pltpu.CompilerParams(
            collective_id=0, has_side_effects=True, vmem_limit_bytes=48 * 1024 * 1024
        ),
    )(
        pair_state.reshape(rows * cols, width),
        in_gain.reshape(1, width),
        left_weight,
        right_weight,
        left_gate,
        right_gate,
        mid_gain.reshape(1, width),
        out_weight,
        out_gate,
    )
    return out.reshape(rows, cols, width)


def solution(mesh):
    north, east = mesh.shape["north"], mesh.shape["east"]
    return jax.shard_map(
        functools.partial(local, north, east),
        mesh=mesh,
        in_specs=(
            P(("trial", "north"), "east", None),
            P(),
            P("trial", None),
            P("trial", None),
            P("trial", None),
            P("trial", None),
            P(),
            P("trial", None),
            P("trial", None),
        ),
        out_specs=P(("trial", "north"), "east", None),
        check_vma=False,
    )
```

```python
import functools

import jax
import jax.numpy as jnp
from jax import lax
from jax.experimental import pallas as pl
from jax.experimental.pallas import tpu as pltpu
from jax.sharding import PartitionSpec as P

MESH = pl.DeviceIdType.MESH
BF16, F32 = jnp.bfloat16, jnp.float32
EPS = 1e-05


def dot_nt(a, b):
    return lax.dot_general(a, b, (((1,), (1,)), ((), ())), preferred_element_type=F32)


def iota(shape, axis):
    return lax.broadcasted_iota(jnp.int32, shape, axis)


def sigmoid(x):
    return jax.nn.sigmoid(x)


def kernel(
    north,
    east,
    rows,
    cols,
    x_hbm,
    in_gain_hbm,
    lw_hbm,
    rw_hbm,
    lg_hbm,
    rg_hbm,
    mid_gain_hbm,
    ow_hbm,
    og_hbm,
    out_ref,
    x_ref,
    in_gain_ref,
    lw_ref,
    rw_ref,
    lg_ref,
    rg_ref,
    mid_gain_ref,
    ow_ref,
    og_ref,
    load_sem,
    ready_ref,
    gate_ref,
    send1,
    recv1,
    left_ref,
    right_ref,
    send2,
    recv2,
    send_sem1,
    recv_sem1,
    send_sem2,
    recv_sem2,
):
    loads = [
        pltpu.make_async_copy(src, dst, load_sem.at[i])
        for i, (src, dst) in enumerate(
            (
                (x_hbm, x_ref),
                (in_gain_hbm, in_gain_ref),
                (lw_hbm, lw_ref),
                (rw_hbm, rw_ref),
                (lg_hbm, lg_ref),
                (rg_hbm, rg_ref),
                (mid_gain_hbm, mid_gain_ref),
                (ow_hbm, ow_ref),
                (og_hbm, og_ref),
            )
        )
    ]
    for load in loads:
        load.start()
    width = x_ref.shape[1]
    group = north * east
    half = rows // 2
    lines = half * cols
    n = lax.axis_index("north")
    e = lax.axis_index("east")
    me = e * north + n

    def device(c, k):
        return lax.rem(e + c, east), lax.rem(n + k, north)

    def each_peer(do):
        for c in range(east):

            def body(k, carry, c=c):
                do(*device(c, k))
                return carry

            lax.fori_loop(1 if c == 0 else 0, north, body, 0)

    barrier = pltpu.get_barrier_semaphore()
    each_peer(
        lambda pe, pn: pl.semaphore_signal(
            barrier, inc=1, device_id={"north": pn, "east": pe}, device_id_type=MESH
        )
    )

    for load in loads:
        load.wait()

    x = x_ref[...].astype(F32)
    centred = x - jnp.mean(x, axis=-1, keepdims=True)
    ready = (
        centred * lax.rsqrt(jnp.mean(centred * centred, axis=-1, keepdims=True) + EPS)
        * in_gain_ref[...]
    ).astype(BF16)
    ready_ref[...] = ready
    both = jnp.concatenate([ready_ref[:lines, :], ready_ref[lines:, :]], axis=1)

    def send_all(src, dst, send_sem, recv_sem):
        dst[me] = src[me]
        each_peer(
            lambda pe, pn: pltpu.make_async_remote_copy(
                src_ref=src.at[pe * north + pn],
                dst_ref=dst.at[me],
                send_sem=send_sem,
                recv_sem=recv_sem,
                device_id={"north": pn, "east": pe},
                device_id_type=MESH,
            ).start()
        )

    def all_of(src, dst, send_sem, recv_sem):
        return pltpu.make_async_remote_copy(
            src_ref=src.at[pl.ds(0, group - 1)],
            dst_ref=dst.at[pl.ds(0, group - 1)],
            send_sem=send_sem,
            recv_sem=recv_sem,
            device_id={"north": n, "east": e},
            device_id_type=MESH,
        )

    r = iota((4 * group, width), 0)
    d = iota((4 * group, width), 1)
    parity = (r & 1) == 0

    def spread(weights, ch):
        picked = 0.0
        for f, w in enumerate(weights):
            pick = (((r >> 1) & 1) == f) & (d == (r >> 2) + ch * group)
            picked = picked + dot_nt(jnp.where(pick, 1.0, 0.0).astype(BF16), w[...])
        return jnp.concatenate(
            [jnp.where(parity, picked, 0.0), jnp.where(parity, 0.0, picked)], axis=1
        ).astype(BF16)

    for ch in range(2):
        value = dot_nt(spread((lw_ref, rw_ref), ch), both)
        gate = dot_nt(spread((lg_ref, rg_ref), ch), both)
        value = (value * sigmoid(gate)).reshape(group, 4, lines)
        send1[ch] = value.astype(BF16)
        if ch == 0:
            pl.semaphore_wait(barrier, group - 1)
        send_all(send1.at[ch], recv1.at[ch], send_sem1.at[ch], recv_sem1.at[ch])

    gate_ref[...] = sigmoid(
        jnp.dot(ready_ref[...], og_ref[...], preferred_element_type=F32)
    )
    left_ref[...] = jnp.zeros_like(left_ref)
    right_ref[...] = jnp.zeros_like(right_ref)

    per = north // east * 2
    for ch in range(2):
        all_of(send1.at[ch], recv1.at[ch], send_sem1.at[ch], recv_sem1.at[ch]).wait_recv()
        for s in range(east):
            lines_l = recv1[ch, north * s : north * (s + 1), 0:2, :].reshape(2 * north, lines)
            lines_r = recv1[ch, north * s : north * (s + 1), 2:4, :].reshape(2 * north, lines)
            for i in range(half):
                left_ref[2 * north * i : 2 * north * (i + 1), 128 * s : 128 * s + cols] = (
                    lines_l[:, cols * i : cols * (i + 1)]
                )
                piece = lines_r[:, cols * i : cols * (i + 1)]
                for t in range(east):
                    right_ref[128 * t + per * i : 128 * t + per * (i + 1), 128 * s : 128 * s + cols] = (
                        piece[per * t : per * (t + 1)]
                    )
        mixed = dot_nt(left_ref[...], right_ref[...]) * (cols * east) ** (-0.5)
        for t in range(east):
            strip = jnp.concatenate(
                [
                    mixed[2 * north * i : 2 * north * (i + 1), 128 * t : 128 * t + cols]
                    for i in range(half)
                ],
                axis=1,
            )
            send2[ch, north * t : north * (t + 1)] = strip.reshape(north, 2, lines).astype(BF16)
        send_all(send2.at[ch], recv2.at[ch], send_sem2.at[ch], recv_sem2.at[ch])

    mid_gain = jnp.broadcast_to(mid_gain_ref[...], (width, width)).T
    mid_gain = jnp.broadcast_to(mid_gain[:, None, :], (width, 2, width)).reshape(2 * width, width)
    mid_gain = jnp.concatenate([mid_gain] * 3, axis=1)
    weight = ow_ref[...].astype(F32)
    weight = jnp.broadcast_to(weight[:, None, :], (width, 2, width)).reshape(2 * width, width)
    first = (iota((2 * width, width), 0) & 1) == 0
    weight = jnp.concatenate(
        [jnp.where(first, weight, 0.0), jnp.where(first, 0.0, weight)], axis=1
    ).astype(BF16)
    tile = 4 * cols
    lane = iota((tile, tile), 1)
    block = jnp.where(lane >= 2 * cols, 2, 0)
    block = block + jnp.where(lane - block * cols >= cols, 1, 0)
    rest = lane - block * cols
    target = block * cols + ((rest & (per - 1)) >> 1) * rows + (rest & 1) * half + (rest >> 3)
    order = jnp.where(iota((tile, tile), 0) == target, 1.0, 0.0).astype(BF16)

    for ch in range(2):
        all_of(send2.at[ch], recv2.at[ch], send_sem2.at[ch], recv_sem2.at[ch]).wait_recv()

    def fold(total):
        total = jnp.sum(total.reshape(2 * width // 8, 8, tile), axis=0)
        total = total + pltpu.roll(total, 4, 0)
        total = total + pltpu.roll(total, 2, 0)
        return (total * (1.0 / width))[None]

    for g in range(lines // tile):
        lanes = slice(g * tile, (g + 1) * tile)
        mixed = recv2[:, :, :, lanes].reshape(2 * width, tile).astype(F32)
        centred = mixed.reshape(2 * width // 8, 8, tile) - fold(mixed)
        scale = lax.rsqrt(fold((centred * centred).reshape(2 * width, tile)) + EPS)
        scaled = ((centred * scale).reshape(2 * width, tile) * mid_gain).astype(BF16)
        turned = dot_nt(order, scaled).astype(BF16)
        result = jnp.dot(turned, weight, preferred_element_type=F32)
        for h in range(2):
            at = slice(h * lines + g * tile, h * lines + (g + 1) * tile)
            out_ref[at, :] = (
                result[:, h * width : (h + 1) * width] * gate_ref[at, :]
            ).astype(BF16)

    for ch in range(2):
        for src, dst, a, b in (
            (send1, recv1, send_sem1, recv_sem1),
            (send2, recv2, send_sem2, recv_sem2),
        ):
            all_of(src.at[ch], dst.at[ch], a.at[ch], b.at[ch]).wait_send()


def local(
    north,
    east,
    pair_state,
    in_gain,
    left_weight,
    right_weight,
    left_gate,
    right_gate,
    mid_gain,
    out_weight,
    out_gate,
):
    rows, cols, width = pair_state.shape
    lines = rows // 2 * cols
    group = north * east
    vmem = pl.BlockSpec(memory_space=pltpu.VMEM)
    out = pl.pallas_call(
        functools.partial(kernel, north, east, rows, cols),
        out_shape=jax.ShapeDtypeStruct((rows * cols, width), BF16),
        in_specs=[pl.BlockSpec(memory_space=pltpu.HBM)] * 9,
        out_specs=vmem,
        scratch_shapes=[
            pltpu.VMEM((rows * cols, width), BF16),
            pltpu.VMEM((1, width), F32),
            pltpu.VMEM((width, width), BF16),
            pltpu.VMEM((width, width), BF16),
            pltpu.VMEM((width, width), BF16),
            pltpu.VMEM((width, width), BF16),
            pltpu.VMEM((1, width), F32),
            pltpu.VMEM((width, width), BF16),
            pltpu.VMEM((width, width), BF16),
            pltpu.SemaphoreType.DMA((9,)),
            pltpu.VMEM((rows * cols, width), BF16),
            pltpu.VMEM((rows * cols, width), F32),
            pltpu.VMEM((2, group, 4, lines), BF16),
            pltpu.VMEM((2, group, 4, lines), BF16),
            pltpu.VMEM((rows * north, 128 * east), BF16),
            pltpu.VMEM((128 * east, 128 * east), BF16),
            pltpu.VMEM((2, group, 2, lines), BF16),
            pltpu.VMEM((2, group, 2, lines), BF16),
            pltpu.SemaphoreType.DMA((2,)),
            pltpu.SemaphoreType.DMA((2,)),
            pltpu.SemaphoreType.DMA((2,)),
            pltpu.SemaphoreType.DMA((2,)),
        ],
        compiler_params=pltpu.CompilerParams(
            collective_id=0, has_side_effects=True, vmem_limit_bytes=48 * 1024 * 1024
        ),
    )(
        pair_state.reshape(rows * cols, width),
        in_gain.reshape(1, width),
        left_weight,
        right_weight,
        left_gate,
        right_gate,
        mid_gain.reshape(1, width),
        out_weight,
        out_gate,
    )
    return out.reshape(rows, cols, width)


def solution(mesh):
    north, east = mesh.shape["north"], mesh.shape["east"]
    return jax.shard_map(
        functools.partial(local, north, east),
        mesh=mesh,
        in_specs=(
            P(("trial", "north"), "east", None),
            P(),
            P("trial", None),
            P("trial", None),
            P("trial", None),
            P("trial", None),
            P(),
            P("trial", None),
            P("trial", None),
        ),
        out_specs=P(("trial", "north"), "east", None),
        check_vma=False,
    )
```

```python
import functools

import jax
import jax.numpy as jnp
from jax import lax
from jax.experimental import pallas as pl
from jax.experimental.pallas import tpu as pltpu
from jax.sharding import PartitionSpec as P

MESH = pl.DeviceIdType.MESH
BF16, F32 = jnp.bfloat16, jnp.float32
EPS = 1e-05


def dot_nt(a, b):
    return lax.dot_general(a, b, (((1,), (1,)), ((), ())), preferred_element_type=F32)


def iota(shape, axis):
    return lax.broadcasted_iota(jnp.int32, shape, axis)


def sigmoid(x):
    return jax.nn.sigmoid(x)


def kernel(
    north,
    east,
    rows,
    cols,
    x_hbm,
    in_gain_hbm,
    lw_hbm,
    rw_hbm,
    lg_hbm,
    rg_hbm,
    mid_gain_hbm,
    ow_hbm,
    og_hbm,
    out_ref,
    x_ref,
    in_gain_ref,
    lw_ref,
    rw_ref,
    lg_ref,
    rg_ref,
    mid_gain_ref,
    ow_ref,
    og_ref,
    load_sem,
    ready_ref,
    gate_ref,
    send1,
    recv1,
    left_ref,
    right_ref,
    send2,
    recv2,
    send_sem1,
    recv_sem1,
    send_sem2,
    recv_sem2,
):
    loads = [
        pltpu.make_async_copy(src, dst, load_sem.at[i])
        for i, (src, dst) in enumerate(
            (
                (x_hbm, x_ref),
                (in_gain_hbm, in_gain_ref),
                (lw_hbm, lw_ref),
                (rw_hbm, rw_ref),
                (lg_hbm, lg_ref),
                (rg_hbm, rg_ref),
                (mid_gain_hbm, mid_gain_ref),
                (ow_hbm, ow_ref),
                (og_hbm, og_ref),
            )
        )
    ]
    for load in loads:
        load.start()
    width = x_ref.shape[1]
    group = north * east
    half = rows // 2
    lines = half * cols
    n = lax.axis_index("north")
    e = lax.axis_index("east")
    me = e * north + n

    def device(c, k):
        return lax.rem(e + c, east), lax.rem(n + k, north)

    def each_peer(do):
        for c in range(east):

            def body(k, carry, c=c):
                do(*device(c, k))
                return carry

            lax.fori_loop(1 if c == 0 else 0, north, body, 0)

    barrier = pltpu.get_barrier_semaphore()
    each_peer(
        lambda pe, pn: pl.semaphore_signal(
            barrier, inc=1, device_id={"north": pn, "east": pe}, device_id_type=MESH
        )
    )

    for load in loads:
        load.wait()

    x = x_ref[...].astype(F32)
    centred = x - jnp.mean(x, axis=-1, keepdims=True)
    ready = (
        centred * lax.rsqrt(jnp.mean(centred * centred, axis=-1, keepdims=True) + EPS)
        * in_gain_ref[...]
    ).astype(BF16)
    ready_ref[...] = ready
    both = jnp.concatenate([ready_ref[:lines, :], ready_ref[lines:, :]], axis=1)

    def send_all(src, dst, send_sem, recv_sem):
        dst[me] = src[me]
        each_peer(
            lambda pe, pn: pltpu.make_async_remote_copy(
                src_ref=src.at[pe * north + pn],
                dst_ref=dst.at[me],
                send_sem=send_sem,
                recv_sem=recv_sem,
                device_id={"north": pn, "east": pe},
                device_id_type=MESH,
            ).start()
        )

    def all_of(src, dst, send_sem, recv_sem):
        return pltpu.make_async_remote_copy(
            src_ref=src.at[pl.ds(0, group - 1)],
            dst_ref=dst.at[pl.ds(0, group - 1)],
            send_sem=send_sem,
            recv_sem=recv_sem,
            device_id={"north": n, "east": e},
            device_id_type=MESH,
        )

    r = iota((4 * group, width), 0)
    d = iota((4 * group, width), 1)
    parity = (r & 1) == 0

    def spread(weights, ch):
        picked = 0.0
        for f, w in enumerate(weights):
            pick = (((r >> 1) & 1) == f) & (d == (r >> 2) + ch * group)
            picked = picked + dot_nt(jnp.where(pick, 1.0, 0.0).astype(BF16), w[...])
        return jnp.concatenate(
            [jnp.where(parity, picked, 0.0), jnp.where(parity, 0.0, picked)], axis=1
        ).astype(BF16)

    for ch in range(2):
        value = dot_nt(spread((lw_ref, rw_ref), ch), both)
        gate = dot_nt(spread((lg_ref, rg_ref), ch), both)
        value = (value * sigmoid(gate)).reshape(group, 4, lines)
        send1[ch] = value.astype(BF16)
        if ch == 0:
            pl.semaphore_wait(barrier, group - 1)
        send_all(send1.at[ch], recv1.at[ch], send_sem1.at[ch], recv_sem1.at[ch])

    gate_ref[...] = sigmoid(
        jnp.dot(ready_ref[...], og_ref[...], preferred_element_type=F32)
    )
    left_ref[...] = jnp.zeros_like(left_ref)
    right_ref[...] = jnp.zeros_like(right_ref)

    per = north // east * 2
    for ch in range(2):
        all_of(send1.at[ch], recv1.at[ch], send_sem1.at[ch], recv_sem1.at[ch]).wait_recv()
        for s in range(east):
            lines_l = recv1[ch, north * s : north * (s + 1), 0:2, :].reshape(2 * north, lines)
            lines_r = recv1[ch, north * s : north * (s + 1), 2:4, :].reshape(2 * north, lines)
            for i in range(half):
                left_ref[2 * north * i : 2 * north * (i + 1), 128 * s : 128 * s + cols] = (
                    lines_l[:, cols * i : cols * (i + 1)]
                )
                piece = lines_r[:, cols * i : cols * (i + 1)]
                for t in range(east):
                    right_ref[128 * t + per * i : 128 * t + per * (i + 1), 128 * s : 128 * s + cols] = (
                        piece[per * t : per * (t + 1)]
                    )
        mixed = dot_nt(left_ref[...], right_ref[...]) * (cols * east) ** (-0.5)
        for t in range(east):
            strip = jnp.concatenate(
                [
                    mixed[2 * north * i : 2 * north * (i + 1), 128 * t : 128 * t + cols]
                    for i in range(half)
                ],
                axis=1,
            )
            send2[ch, north * t : north * (t + 1)] = strip.reshape(north, 2, lines).astype(BF16)
        send_all(send2.at[ch], recv2.at[ch], send_sem2.at[ch], recv_sem2.at[ch])

    mid_gain = jnp.broadcast_to(mid_gain_ref[...], (width, width)).T
    mid_gain = jnp.broadcast_to(mid_gain[:, None, :], (width, 2, width)).reshape(2 * width, width)
    mid_gain = jnp.concatenate([mid_gain] * 3, axis=1)
    weight = ow_ref[...].astype(F32)
    weight = jnp.broadcast_to(weight[:, None, :], (width, 2, width)).reshape(2 * width, width)
    first = (iota((2 * width, width), 0) & 1) == 0
    weight = jnp.concatenate(
        [jnp.where(first, weight, 0.0), jnp.where(first, 0.0, weight)], axis=1
    ).astype(BF16)
    tile = 4 * cols
    lane = iota((tile, tile), 1)
    block = jnp.where(lane >= 2 * cols, 2, 0)
    block = block + jnp.where(lane - block * cols >= cols, 1, 0)
    rest = lane - block * cols
    target = block * cols + ((rest & (per - 1)) >> 1) * rows + (rest & 1) * half + (rest >> 3)
    order = jnp.where(iota((tile, tile), 0) == target, 1.0, 0.0).astype(BF16)

    for ch in range(2):
        all_of(send2.at[ch], recv2.at[ch], send_sem2.at[ch], recv_sem2.at[ch]).wait_recv()

    def fold(total):
        total = jnp.sum(total.reshape(2 * width // 8, 8, tile), axis=0)
        total = total + pltpu.roll(total, 4, 0)
        total = total + pltpu.roll(total, 2, 0)
        return (total * (1.0 / width))[None]

    for g in range(lines // tile):
        lanes = slice(g * tile, (g + 1) * tile)
        mixed = recv2[:, :, :, lanes].reshape(2 * width, tile).astype(F32)
        centred = mixed.reshape(2 * width // 8, 8, tile) - fold(mixed)
        scale = lax.rsqrt(fold((centred * centred).reshape(2 * width, tile)) + EPS)
        scaled = ((centred * scale).reshape(2 * width, tile) * mid_gain).astype(BF16)
        turned = dot_nt(order, scaled).astype(BF16)
        result = jnp.dot(turned, weight, preferred_element_type=F32)
        for h in range(2):
            at = slice(h * lines + g * tile, h * lines + (g + 1) * tile)
            out_ref[at, :] = (
                result[:, h * width : (h + 1) * width] * gate_ref[at, :]
            ).astype(BF16)

    for ch in range(2):
        for src, dst, a, b in (
            (send1, recv1, send_sem1, recv_sem1),
            (send2, recv2, send_sem2, recv_sem2),
        ):
            all_of(src.at[ch], dst.at[ch], a.at[ch], b.at[ch]).wait_send()


def local(
    north,
    east,
    pair_state,
    in_gain,
    left_weight,
    right_weight,
    left_gate,
    right_gate,
    mid_gain,
    out_weight,
    out_gate,
):
    rows, cols, width = pair_state.shape
    lines = rows // 2 * cols
    group = north * east
    vmem = pl.BlockSpec(memory_space=pltpu.VMEM)
    out = pl.pallas_call(
        functools.partial(kernel, north, east, rows, cols),
        out_shape=jax.ShapeDtypeStruct((rows * cols, width), BF16),
        in_specs=[pl.BlockSpec(memory_space=pltpu.HBM)] * 9,
        out_specs=vmem,
        scratch_shapes=[
            pltpu.VMEM((rows * cols, width), BF16),
            pltpu.VMEM((1, width), F32),
            pltpu.VMEM((width, width), BF16),
            pltpu.VMEM((width, width), BF16),
            pltpu.VMEM((width, width), BF16),
            pltpu.VMEM((width, width), BF16),
            pltpu.VMEM((1, width), F32),
            pltpu.VMEM((width, width), BF16),
            pltpu.VMEM((width, width), BF16),
            pltpu.SemaphoreType.DMA((9,)),
            pltpu.VMEM((rows * cols, width), BF16),
            pltpu.VMEM((rows * cols, width), F32),
            pltpu.VMEM((2, group, 4, lines), BF16),
            pltpu.VMEM((2, group, 4, lines), BF16),
            pltpu.VMEM((rows * north, 128 * east), BF16),
            pltpu.VMEM((128 * east, 128 * east), BF16),
            pltpu.VMEM((2, group, 2, lines), BF16),
            pltpu.VMEM((2, group, 2, lines), BF16),
            pltpu.SemaphoreType.DMA((2,)),
            pltpu.SemaphoreType.DMA((2,)),
            pltpu.SemaphoreType.DMA((2,)),
            pltpu.SemaphoreType.DMA((2,)),
        ],
        compiler_params=pltpu.CompilerParams(
            collective_id=0, has_side_effects=True, vmem_limit_bytes=67_043_328
        ),
    )(
        pair_state.reshape(rows * cols, width),
        in_gain.reshape(1, width),
        left_weight,
        right_weight,
        left_gate,
        right_gate,
        mid_gain.reshape(1, width),
        out_weight,
        out_gate,
    )
    return out.reshape(rows, cols, width)


def solution(mesh):
    north, east = mesh.shape["north"], mesh.shape["east"]
    return jax.shard_map(
        functools.partial(local, north, east),
        mesh=mesh,
        in_specs=(
            P(("trial", "north"), "east", None),
            P(),
            P("trial", None),
            P("trial", None),
            P("trial", None),
            P("trial", None),
            P(),
            P("trial", None),
            P("trial", None),
        ),
        out_specs=P(("trial", "north"), "east", None),
        check_vma=False,
    )
```

```python
import functools

import jax
import jax.numpy as jnp
from jax import lax
from jax.experimental import pallas as pl
from jax.experimental.pallas import tpu as pltpu
from jax.sharding import PartitionSpec as P

MESH = pl.DeviceIdType.MESH
BF16, F32 = jnp.bfloat16, jnp.float32
EPS = 1e-05


def dot_nt(a, b):
    return lax.dot_general(a, b, (((1,), (1,)), ((), ())), preferred_element_type=F32)


def iota(shape, axis):
    return lax.broadcasted_iota(jnp.int32, shape, axis)


def sigmoid(x):
    return jax.nn.sigmoid(x)


def kernel(
    north,
    east,
    rows,
    cols,
    x_hbm,
    in_gain_hbm,
    lw_hbm,
    rw_hbm,
    lg_hbm,
    rg_hbm,
    mid_gain_hbm,
    ow_hbm,
    og_hbm,
    out_ref,
    x_ref,
    in_gain_ref,
    lw_ref,
    rw_ref,
    lg_ref,
    rg_ref,
    mid_gain_ref,
    ow_ref,
    og_ref,
    load_sem,
    ready_ref,
    gate_ref,
    send1,
    recv1,
    left_ref,
    right_ref,
    send2,
    recv2,
    send_sem1,
    recv_sem1,
    send_sem2,
    recv_sem2,
):
    loads = [
        pltpu.make_async_copy(src, dst, load_sem.at[i])
        for i, (src, dst) in enumerate(
            (
                (x_hbm, x_ref),
                (in_gain_hbm, in_gain_ref),
                (lw_hbm, lw_ref),
                (rw_hbm, rw_ref),
                (lg_hbm, lg_ref),
                (rg_hbm, rg_ref),
                (mid_gain_hbm, mid_gain_ref),
                (ow_hbm, ow_ref),
                (og_hbm, og_ref),
            )
        )
    ]
    for load in loads:
        load.start()
    width = x_ref.shape[1]
    group = north * east
    half = rows // 2
    lines = half * cols
    n = lax.axis_index("north")
    e = lax.axis_index("east")
    me = e * north + n

    def device(c, k):
        return lax.rem(e + c, east), lax.rem(n + k, north)

    def each_peer(do):
        for c in range(east):

            def body(k, carry, c=c):
                do(*device(c, k))
                return carry

            lax.fori_loop(1 if c == 0 else 0, north, body, 0)

    barrier = pltpu.get_barrier_semaphore()
    each_peer(
        lambda pe, pn: pl.semaphore_signal(
            barrier, inc=1, device_id={"north": pn, "east": pe}, device_id_type=MESH
        )
    )

    for load in loads:
        load.wait()

    x = x_ref[...].astype(F32)
    centred = x - jnp.mean(x, axis=-1, keepdims=True)
    ready = (
        centred * lax.rsqrt(jnp.mean(centred * centred, axis=-1, keepdims=True) + EPS)
        * in_gain_ref[...]
    ).astype(BF16)
    ready_ref[...] = ready
    both = jnp.concatenate([ready_ref[:lines, :], ready_ref[lines:, :]], axis=1)

    def send_all(src, dst, send_sem, recv_sem):
        dst[me] = src[me]
        each_peer(
            lambda pe, pn: pltpu.make_async_remote_copy(
                src_ref=src.at[pe * north + pn],
                dst_ref=dst.at[me],
                send_sem=send_sem,
                recv_sem=recv_sem,
                device_id={"north": pn, "east": pe},
                device_id_type=MESH,
            ).start()
        )

    def all_of(src, dst, send_sem, recv_sem):
        return pltpu.make_async_remote_copy(
            src_ref=src.at[pl.ds(0, group - 1)],
            dst_ref=dst.at[pl.ds(0, group - 1)],
            send_sem=send_sem,
            recv_sem=recv_sem,
            device_id={"north": n, "east": e},
            device_id_type=MESH,
        )

    r = iota((4 * group, width), 0)
    d = iota((4 * group, width), 1)
    parity = (r & 1) == 0

    def spread(weights, ch):
        picked = 0.0
        for f, w in enumerate(weights):
            pick = (((r >> 1) & 1) == f) & (d == (r >> 2) + ch * group)
            picked = picked + dot_nt(jnp.where(pick, 1.0, 0.0).astype(BF16), w[...])
        return jnp.concatenate(
            [jnp.where(parity, picked, 0.0), jnp.where(parity, 0.0, picked)], axis=1
        ).astype(BF16)

    for ch in range(2):
        value = dot_nt(spread((lw_ref, rw_ref), ch), both)
        gate = dot_nt(spread((lg_ref, rg_ref), ch), both)
        value = (value * sigmoid(gate)).reshape(group, 4, lines)
        send1[ch] = value.astype(BF16)
        if ch == 0:
            pl.semaphore_wait(barrier, group - 1)
        send_all(send1.at[ch], recv1.at[ch], send_sem1.at[ch], recv_sem1.at[ch])

    gate_ref[...] = sigmoid(
        jnp.dot(ready_ref[...], og_ref[...], preferred_element_type=F32)
    )
    left_ref[...] = jnp.zeros_like(left_ref)
    right_ref[...] = jnp.zeros_like(right_ref)

    per = north // east * 2
    for ch in range(2):
        all_of(send1.at[ch], recv1.at[ch], send_sem1.at[ch], recv_sem1.at[ch]).wait_recv()
        for s in range(east):
            lines_l = recv1[ch, north * s : north * (s + 1), 0:2, :].reshape(2 * north, lines)
            lines_r = recv1[ch, north * s : north * (s + 1), 2:4, :].reshape(2 * north, lines)
            for i in range(half):
                left_ref[2 * north * i : 2 * north * (i + 1), 128 * s : 128 * s + cols] = (
                    lines_l[:, cols * i : cols * (i + 1)]
                )
                piece = lines_r[:, cols * i : cols * (i + 1)]
                for t in range(east):
                    right_ref[128 * t + per * i : 128 * t + per * (i + 1), 128 * s : 128 * s + cols] = (
                        piece[per * t : per * (t + 1)]
                    )
        mixed = dot_nt(left_ref[...], right_ref[...]) * (cols * east) ** (-0.5)
        for t in range(east):
            strip = jnp.concatenate(
                [
                    mixed[2 * north * i : 2 * north * (i + 1), 128 * t : 128 * t + cols]
                    for i in range(half)
                ],
                axis=1,
            )
            send2[ch, north * t : north * (t + 1)] = strip.reshape(north, 2, lines).astype(BF16)
        send_all(send2.at[ch], recv2.at[ch], send_sem2.at[ch], recv_sem2.at[ch])

    mid_gain = jnp.broadcast_to(mid_gain_ref[...], (width, width)).T
    mid_gain = jnp.broadcast_to(mid_gain[:, None, :], (width, 2, width)).reshape(2 * width, width)
    mid_gain = jnp.concatenate([mid_gain] * 3, axis=1)
    weight = ow_ref[...].astype(F32)
    weight = jnp.broadcast_to(weight[:, None, :], (width, 2, width)).reshape(2 * width, width)
    first = (iota((2 * width, width), 0) & 1) == 0
    weight = jnp.concatenate(
        [jnp.where(first, weight, 0.0), jnp.where(first, 0.0, weight)], axis=1
    ).astype(BF16)
    tile = 4 * cols
    lane = iota((tile, tile), 1)
    block = jnp.where(lane >= 2 * cols, 2, 0)
    block = block + jnp.where(lane - block * cols >= cols, 1, 0)
    rest = lane - block * cols
    target = block * cols + ((rest & (per - 1)) >> 1) * rows + (rest & 1) * half + (rest >> 3)
    order = jnp.where(iota((tile, tile), 0) == target, 1.0, 0.0).astype(BF16)

    for ch in range(2):
        all_of(send2.at[ch], recv2.at[ch], send_sem2.at[ch], recv_sem2.at[ch]).wait_recv()

    def fold(total):
        total = jnp.sum(total.reshape(2 * width // 8, 8, tile), axis=0)
        total = total + pltpu.roll(total, 4, 0)
        total = total + pltpu.roll(total, 2, 0)
        return (total * (1.0 / width))[None]

    for g in range(lines // tile):
        lanes = slice(g * tile, (g + 1) * tile)
        mixed = recv2[:, :, :, lanes].reshape(2 * width, tile).astype(F32)
        centred = mixed.reshape(2 * width // 8, 8, tile) - fold(mixed)
        scale = lax.rsqrt(fold((centred * centred).reshape(2 * width, tile)) + EPS)
        scaled = ((centred * scale).reshape(2 * width, tile) * mid_gain).astype(BF16)
        turned = dot_nt(order, scaled).astype(BF16)
        result = jnp.dot(turned, weight, preferred_element_type=F32)
        for h in range(2):
            at = slice(h * lines + g * tile, h * lines + (g + 1) * tile)
            out_ref[at, :] = (
                result[:, h * width : (h + 1) * width] * gate_ref[at, :]
            ).astype(BF16)

    for ch in range(2):
        for src, dst, a, b in (
            (send1, recv1, send_sem1, recv_sem1),
            (send2, recv2, send_sem2, recv_sem2),
        ):
            all_of(src.at[ch], dst.at[ch], a.at[ch], b.at[ch]).wait_send()


def local(
    north,
    east,
    pair_state,
    in_gain,
    left_weight,
    right_weight,
    left_gate,
    right_gate,
    mid_gain,
    out_weight,
    out_gate,
):
    rows, cols, width = pair_state.shape
    lines = rows // 2 * cols
    group = north * east
    vmem = pl.BlockSpec(memory_space=pltpu.VMEM)
    out = pl.pallas_call(
        functools.partial(kernel, north, east, rows, cols),
        out_shape=pltpu.VMEM((rows * cols, width), BF16),
        in_specs=[pl.BlockSpec(memory_space=pltpu.HBM)] * 9,
        out_specs=vmem,
        scratch_shapes=[
            pltpu.VMEM((rows * cols, width), BF16),
            pltpu.VMEM((1, width), F32),
            pltpu.VMEM((width, width), BF16),
            pltpu.VMEM((width, width), BF16),
            pltpu.VMEM((width, width), BF16),
            pltpu.VMEM((width, width), BF16),
            pltpu.VMEM((1, width), F32),
            pltpu.VMEM((width, width), BF16),
            pltpu.VMEM((width, width), BF16),
            pltpu.SemaphoreType.DMA((9,)),
            pltpu.VMEM((rows * cols, width), BF16),
            pltpu.VMEM((rows * cols, width), F32),
            pltpu.VMEM((2, group, 4, lines), BF16),
            pltpu.VMEM((2, group, 4, lines), BF16),
            pltpu.VMEM((rows * north, 128 * east), BF16),
            pltpu.VMEM((128 * east, 128 * east), BF16),
            pltpu.VMEM((2, group, 2, lines), BF16),
            pltpu.VMEM((2, group, 2, lines), BF16),
            pltpu.SemaphoreType.DMA((2,)),
            pltpu.SemaphoreType.DMA((2,)),
            pltpu.SemaphoreType.DMA((2,)),
            pltpu.SemaphoreType.DMA((2,)),
        ],
        compiler_params=pltpu.CompilerParams(
            collective_id=0, has_side_effects=True, vmem_limit_bytes=48 * 1024 * 1024
        ),
    )(
        *(
            pltpu.with_memory_space_constraint(a, pltpu.HBM)
            for a in (
                pair_state.reshape(rows * cols, width),
                in_gain.reshape(1, width),
                left_weight,
                right_weight,
                left_gate,
                right_gate,
                mid_gain.reshape(1, width),
                out_weight,
                out_gate,
            )
        )
    )
    return out.reshape(rows, cols, width)


def solution(mesh):
    north, east = mesh.shape["north"], mesh.shape["east"]
    return jax.shard_map(
        functools.partial(local, north, east),
        mesh=mesh,
        in_specs=(
            P(("trial", "north"), "east", None),
            P(),
            P("trial", None),
            P("trial", None),
            P("trial", None),
            P("trial", None),
            P(),
            P("trial", None),
            P("trial", None),
        ),
        out_specs=P(("trial", "north"), "east", None),
        check_vma=False,
    )
```

```python
import functools

import jax
import jax.numpy as jnp
from jax import lax
from jax.experimental import pallas as pl
from jax.experimental.pallas import tpu as pltpu
from jax.sharding import PartitionSpec as P

MESH = pl.DeviceIdType.MESH
BF16, F32 = jnp.bfloat16, jnp.float32
Y, X = 4, 2
EPS = 1e-05


def dot_nt(a, b):
    return lax.dot_general(a, b, (((1,), (1,)), ((), ())), preferred_element_type=F32)


def iota(shape, axis):
    return lax.broadcasted_iota(jnp.int32, shape, axis)


def sigmoid(x):
    return jax.nn.sigmoid(x)


def kernel(
    north,
    east,
    rows,
    cols,
    x_hbm,
    in_gain_hbm,
    lw_hbm,
    rw_hbm,
    lg_hbm,
    rg_hbm,
    mid_gain_hbm,
    ow_hbm,
    og_hbm,
    out_ref,
    x_ref,
    in_gain_ref,
    lw_ref,
    rw_ref,
    lg_ref,
    rg_ref,
    mid_gain_ref,
    ow_ref,
    og_ref,
    load_sem,
    ready_ref,
    gate_ref,
    send1,
    recv1,
    left_ref,
    right_ref,
    send2,
    recv2,
    send_sem1,
    recv_sem1,
    send_sem2,
    recv_sem2,
    known,
    spread_ref,
):
    loads = [
        pltpu.make_async_copy(src, dst, load_sem.at[i])
        for i, (src, dst) in enumerate(
            (
                (x_hbm, x_ref),
                (in_gain_hbm, in_gain_ref),
                (lw_hbm, lw_ref),
                (rw_hbm, rw_ref),
                (lg_hbm, lg_ref),
                (rg_hbm, rg_ref),
                (mid_gain_hbm, mid_gain_ref),
                (ow_hbm, ow_ref),
                (og_hbm, og_ref),
            )
        )
    ]
    for load in loads:
        load.start()
    width = x_ref.shape[1]
    group = north * east
    half = rows // 2
    lines = half * cols
    n = lax.axis_index("north")
    e = lax.axis_index("east")
    me = e * north + n

    at_z, at_y, at_x = n // (Y * X) * east + e, lax.rem(n // X, Y), lax.rem(n, X)
    depth = group // (Y * X)
    everyone = [(a, b, c) for a in range(depth) for b in range(Y) for c in range(X)][1:]
    everyone.sort(key=lambda o: -min(o[0], depth - o[0]) - min(o[1], Y - o[1]) - 2 * o[2])
    columns = [o for o in everyone if o[0] == 0]
    near = [o for o in everyone if o in columns or o[1:] == (0, 0)]
    rest = [o for o in everyone if o not in near]

    def each_peer(offsets, do):
        for dz, dy, dx in offsets:
            pz = lax.rem(at_z + dz, depth)
            north_of = (pz // east * Y + lax.rem(at_y + dy, Y)) * X + lax.rem(at_x + dx, X)
            east_of = lax.rem(pz, east)
            do(east_of * north + north_of, {"north": north_of, "east": east_of})

    def signal(semaphore, offsets):
        each_peer(
            offsets,
            lambda q, device: pl.semaphore_signal(
                semaphore, inc=1, device_id=device, device_id_type=MESH
            ),
        )

    barrier = pltpu.get_barrier_semaphore()
    signal(barrier, near)

    def send(src, dst, send_sem, recv_sem, offsets):
        each_peer(
            offsets,
            lambda q, device: pltpu.make_async_remote_copy(
                src_ref=src(q),
                dst_ref=dst(me),
                send_sem=send_sem,
                recv_sem=recv_sem,
                device_id=device,
                device_id_type=MESH,
            ).start(),
        )

    def all_of(src, dst, send_sem, recv_sem):
        most = pl.ds(0, group - 1)
        return pltpu.make_async_remote_copy(
            src_ref=src(most),
            dst_ref=dst(most),
            send_sem=send_sem,
            recv_sem=recv_sem,
            device_id={"north": n, "east": e},
            device_id_type=MESH,
        )

    def leg1(ch):
        return (
            lambda q: send1.at[ch, q],
            lambda q: recv1.at[ch, q],
            send_sem1.at[ch],
            recv_sem1.at[ch],
        )

    tile = 4 * cols
    parts = ((0, 0, 3), (1, 0, 3))

    def leg2(i):
        ch, start, stop = parts[i]
        lanes = pl.ds(start * tile, (stop - start) * tile)
        return (
            lambda q: send2.at[ch, q, :, lanes],
            lambda q: recv2.at[ch, q, :, lanes],
            send_sem2.at[i],
            recv_sem2.at[i],
        )

    for load in loads[1:]:
        load.wait()
    r = iota((4 * group, width), 0)
    d = iota((4 * group, width), 1)
    parity = (r & 1) == 0

    def spread(weights, ch):
        picked = 0.0
        for f, w in enumerate(weights):
            pick = (((r >> 1) & 1) == f) & (d == (r >> 2) + ch * group)
            picked = picked + dot_nt(jnp.where(pick, 1.0, 0.0).astype(BF16), w[...])
        return jnp.concatenate(
            [jnp.where(parity, picked, 0.0), jnp.where(parity, 0.0, picked)], axis=1
        ).astype(BF16)

    for ch in range(2):
        spread_ref[2 * ch] = spread((lw_ref, rw_ref), ch)
        spread_ref[2 * ch + 1] = spread((lg_ref, rg_ref), ch)

    loads[0].wait()
    x = x_ref[...].astype(F32)
    centred = x - jnp.mean(x, axis=-1, keepdims=True)
    ready = (
        centred * lax.rsqrt(jnp.mean(centred * centred, axis=-1, keepdims=True) + EPS)
        * in_gain_ref[...]
    ).astype(BF16)
    ready_ref[...] = ready
    both = jnp.concatenate([ready_ref[:lines, :], ready_ref[lines:, :]], axis=1)

    for ch in range(2):
        value = dot_nt(spread_ref[2 * ch], both) * sigmoid(dot_nt(spread_ref[2 * ch + 1], both))
        send1[ch] = value.reshape(group, 4, lines).astype(BF16)
        if ch == 0:
            pl.semaphore_wait(barrier, len(near))
            for k, (dz, dy, dx) in enumerate(columns):
                signal(known.at[k], [(0, (Y - dy) % Y, (X - dx) % X)])
        recv1[ch, me] = send1[ch, me]
        send(*leg1(ch), near)
    for k, offset in sorted(enumerate(columns), key=lambda c: everyone.index(c[1]), reverse=True):
        pl.semaphore_wait(known.at[k], 1)
        send(*leg1(0), [o for o in rest if o[1:] == offset[1:]])
    send(*leg1(1), rest)

    gate_ref[...] = sigmoid(
        jnp.dot(ready_ref[...], og_ref[...], preferred_element_type=F32)
    )
    left_ref[...] = jnp.zeros_like(left_ref)
    right_ref[...] = jnp.zeros_like(right_ref)

    per = north // east * 2
    for ch in range(2):
        all_of(*leg1(ch)).wait_recv()
        for s in range(east):
            lines_l = recv1[ch, north * s : north * (s + 1), 0:2, :].reshape(2 * north, lines)
            lines_r = recv1[ch, north * s : north * (s + 1), 2:4, :].reshape(2 * north, lines)
            for i in range(half):
                left_ref[2 * north * i : 2 * north * (i + 1), 128 * s : 128 * s + cols] = (
                    lines_l[:, cols * i : cols * (i + 1)]
                )
                piece = lines_r[:, cols * i : cols * (i + 1)]
                for t in range(east):
                    right_ref[128 * t + per * i : 128 * t + per * (i + 1), 128 * s : 128 * s + cols] = (
                        piece[per * t : per * (t + 1)]
                    )
        mixed = dot_nt(left_ref[...], right_ref[...]) * (cols * east) ** (-0.5)
        for t in range(east):
            strip = jnp.concatenate(
                [
                    mixed[2 * north * i : 2 * north * (i + 1), 128 * t : 128 * t + cols]
                    for i in range(half)
                ],
                axis=1,
            )
            send2[ch, north * t : north * (t + 1)] = strip.reshape(north, 2, lines).astype(BF16)
        recv2[ch, me] = send2[ch, me]
        for i in range(len(parts)):
            if parts[i][0] == ch:
                send(*leg2(i), everyone)

    mid_gain = jnp.broadcast_to(mid_gain_ref[...], (width, width)).T
    mid_gain = jnp.broadcast_to(mid_gain[:, None, :], (width, 2, width)).reshape(2 * width, width)
    mid_gain = jnp.concatenate([mid_gain] * 3, axis=1)
    weight = ow_ref[...].astype(F32)
    weight = jnp.broadcast_to(weight[:, None, :], (width, 2, width)).reshape(2 * width, width)
    first = (iota((2 * width, width), 0) & 1) == 0
    weight = jnp.concatenate(
        [jnp.where(first, weight, 0.0), jnp.where(first, 0.0, weight)], axis=1
    ).astype(BF16)
    lane = iota((tile, tile), 1)
    block = jnp.where(lane >= 2 * cols, 2, 0)
    block = block + jnp.where(lane - block * cols >= cols, 1, 0)
    rest = lane - block * cols
    target = block * cols + ((rest & (per - 1)) >> 1) * rows + (rest & 1) * half + (rest >> 3)
    order = jnp.where(iota((tile, tile), 0) == target, 1.0, 0.0).astype(BF16)

    def fold(total):
        total = jnp.sum(total.reshape(2 * width // 8, 8, tile), axis=0)
        total = total + pltpu.roll(total, 4, 0)
        total = total + pltpu.roll(total, 2, 0)
        return (total * (1.0 / width))[None]

    for g in range(lines // tile):
        if g == 0:
            all_of(*leg2(0)).wait_recv()
            all_of(*leg2(1)).wait_recv()
        lanes = slice(g * tile, (g + 1) * tile)
        mixed = recv2[:, :, :, lanes].reshape(2 * width, tile).astype(F32)
        centred = mixed.reshape(2 * width // 8, 8, tile) - fold(mixed)
        scale = lax.rsqrt(fold((centred * centred).reshape(2 * width, tile)) + EPS)
        scaled = ((centred * scale).reshape(2 * width, tile) * mid_gain).astype(BF16)
        turned = dot_nt(order, scaled).astype(BF16)
        result = jnp.dot(turned, weight, preferred_element_type=F32)
        for h in range(2):
            at = slice(h * lines + g * tile, h * lines + (g + 1) * tile)
            out_ref[at, :] = (
                result[:, h * width : (h + 1) * width] * gate_ref[at, :]
            ).astype(BF16)

    for ch in range(2):
        all_of(*leg1(ch)).wait_send()
    for i in range(len(parts)):
        all_of(*leg2(i)).wait_send()


def local(
    north,
    east,
    pair_state,
    in_gain,
    left_weight,
    right_weight,
    left_gate,
    right_gate,
    mid_gain,
    out_weight,
    out_gate,
):
    rows, cols, width = pair_state.shape
    lines = rows // 2 * cols
    group = north * east
    vmem = pl.BlockSpec(memory_space=pltpu.VMEM)
    out = pl.pallas_call(
        functools.partial(kernel, north, east, rows, cols),
        out_shape=pltpu.VMEM((rows * cols, width), BF16),
        in_specs=[pl.BlockSpec(memory_space=pltpu.HBM)] * 9,
        out_specs=vmem,
        scratch_shapes=[
            pltpu.VMEM((rows * cols, width), BF16),
            pltpu.VMEM((1, width), F32),
            pltpu.VMEM((width, width), BF16),
            pltpu.VMEM((width, width), BF16),
            pltpu.VMEM((width, width), BF16),
            pltpu.VMEM((width, width), BF16),
            pltpu.VMEM((1, width), F32),
            pltpu.VMEM((width, width), BF16),
            pltpu.VMEM((width, width), BF16),
            pltpu.SemaphoreType.DMA((9,)),
            pltpu.VMEM((rows * cols, width), BF16),
            pltpu.VMEM((rows * cols, width), F32),
            pltpu.VMEM((2, group, 4, lines), BF16),
            pltpu.VMEM((2, group, 4, lines), BF16),
            pltpu.VMEM((rows * north, 128 * east), BF16),
            pltpu.VMEM((128 * east, 128 * east), BF16),
            pltpu.VMEM((2, group, 2, lines), BF16),
            pltpu.VMEM((2, group, 2, lines), BF16),
            pltpu.SemaphoreType.DMA((2,)),
            pltpu.SemaphoreType.DMA((2,)),
            pltpu.SemaphoreType.DMA((2,)),
            pltpu.SemaphoreType.DMA((2,)),
            pltpu.SemaphoreType.REGULAR((Y * X - 1,)),
            pltpu.VMEM((4, 4 * group, 2 * width), BF16),
        ],
        compiler_params=pltpu.CompilerParams(
            collective_id=0, has_side_effects=True, vmem_limit_bytes=48 * 1024 * 1024
        ),
    )(
        *(
            pltpu.with_memory_space_constraint(a, pltpu.HBM)
            for a in (
                pair_state.reshape(rows * cols, width),
                in_gain.reshape(1, width),
                left_weight,
                right_weight,
                left_gate,
                right_gate,
                mid_gain.reshape(1, width),
                out_weight,
                out_gate,
            )
        )
    )
    return out.reshape(rows, cols, width)


def solution(mesh):
    north, east = mesh.shape["north"], mesh.shape["east"]
    return jax.shard_map(
        functools.partial(local, north, east),
        mesh=mesh,
        in_specs=(
            P(("trial", "north"), "east", None),
            P(),
            P("trial", None),
            P("trial", None),
            P("trial", None),
            P("trial", None),
            P(),
            P("trial", None),
            P("trial", None),
        ),
        out_specs=P(("trial", "north"), "east", None),
        check_vma=False,
    )
```

```python
import functools

import jax
import jax.numpy as jnp
from jax import lax
from jax.experimental import pallas as pl
from jax.experimental.pallas import tpu as pltpu
from jax.sharding import PartitionSpec as P

MESH = pl.DeviceIdType.MESH
BF16, F32 = jnp.bfloat16, jnp.float32
Y, X = 4, 2
EPS = 1e-05


def dot_nt(a, b):
    return lax.dot_general(a, b, (((1,), (1,)), ((), ())), preferred_element_type=F32)


def iota(shape, axis):
    return lax.broadcasted_iota(jnp.int32, shape, axis)


def sigmoid(x):
    return jax.nn.sigmoid(x)


def kernel(
    north,
    east,
    rows,
    cols,
    x_hbm,
    in_gain_hbm,
    lw_hbm,
    rw_hbm,
    lg_hbm,
    rg_hbm,
    mid_gain_hbm,
    ow_hbm,
    og_hbm,
    out_ref,
    x_ref,
    in_gain_ref,
    lw_ref,
    rw_ref,
    lg_ref,
    rg_ref,
    mid_gain_ref,
    ow_ref,
    og_ref,
    load_sem,
    ready_ref,
    gate_ref,
    send1,
    recv1,
    left_ref,
    right_ref,
    send2,
    recv2,
    send_sem1,
    recv_sem1,
    send_sem2,
    recv_sem2,
    known,
    spread_ref,
    mixed_ref,
    mean_ref,
    spread0_ref,
):
    loads = [
        pltpu.make_async_copy(src, dst, load_sem.at[i])
        for i, (src, dst) in enumerate(
            (
                (x_hbm, x_ref),
                (in_gain_hbm, in_gain_ref),
                (lw_hbm, lw_ref),
                (rw_hbm, rw_ref),
                (lg_hbm, lg_ref),
                (rg_hbm, rg_ref),
                (mid_gain_hbm, mid_gain_ref),
                (ow_hbm, ow_ref),
                (og_hbm, og_ref),
            )
        )
    ]
    for load in loads:
        load.start()
    width = x_ref.shape[1]
    group = north * east
    half = rows // 2
    lines = half * cols
    n = lax.axis_index("north")
    e = lax.axis_index("east")
    me = e * north + n

    at_z, at_y, at_x = n // (Y * X) * east + e, lax.rem(n // X, Y), lax.rem(n, X)
    depth = group // (Y * X)
    everyone = [(a, b, c) for a in range(depth) for b in range(Y) for c in range(X)][1:]
    everyone.sort(key=lambda o: -min(o[0], depth - o[0]) - min(o[1], Y - o[1]) - 2 * o[2])
    columns = [o for o in everyone if o[0] == 0]
    near = [o for o in everyone if o in columns or o[1:] == (0, 0)]
    rest = [o for o in everyone if o not in near]

    def each_peer(offsets, do):
        for dz, dy, dx in offsets:
            pz = lax.rem(at_z + dz, depth)
            north_of = (pz // east * Y + lax.rem(at_y + dy, Y)) * X + lax.rem(at_x + dx, X)
            east_of = lax.rem(pz, east)
            do(east_of * north + north_of, {"north": north_of, "east": east_of})

    def signal(semaphore, offsets):
        each_peer(
            offsets,
            lambda q, device: pl.semaphore_signal(
                semaphore, inc=1, device_id=device, device_id_type=MESH
            ),
        )

    barrier = pltpu.get_barrier_semaphore()
    signal(barrier, near)

    def send(src, dst, send_sem, recv_sem, offsets):
        each_peer(
            offsets,
            lambda q, device: pltpu.make_async_remote_copy(
                src_ref=src(q),
                dst_ref=dst(me),
                send_sem=send_sem,
                recv_sem=recv_sem,
                device_id=device,
                device_id_type=MESH,
            ).start(),
        )

    def all_of(src, dst, send_sem, recv_sem):
        most = pl.ds(0, group - 1)
        return pltpu.make_async_remote_copy(
            src_ref=src(most),
            dst_ref=dst(most),
            send_sem=send_sem,
            recv_sem=recv_sem,
            device_id={"north": n, "east": e},
            device_id_type=MESH,
        )

    def leg1(ch):
        return (
            lambda q: send1.at[ch, q],
            lambda q: recv1.at[ch, q],
            send_sem1.at[ch],
            recv_sem1.at[ch],
        )

    tile = 4 * cols
    parts = ((0, 0, 3), (1, 0, 3))

    def leg2(i):
        ch, start, stop = parts[i]
        lanes = pl.ds(start * tile, (stop - start) * tile)
        return (
            lambda q: send2.at[ch, q, :, lanes],
            lambda q: recv2.at[ch, q, :, lanes],
            send_sem2.at[i],
            recv_sem2.at[i],
        )

    for load in loads:
        load.wait()
    r = iota((4 * group, width), 0)
    d = iota((4 * group, width), 1)
    parity = (r & 1) == 0

    def spread(weights, ch):
        picked = 0.0
        for f, w in enumerate(weights):
            pick = (((r >> 1) & 1) == f) & (d == (r >> 2) + ch * group)
            picked = picked + dot_nt(jnp.where(pick, 1.0, 0.0).astype(BF16), w[...])
        return jnp.concatenate(
            [jnp.where(parity, picked, 0.0), jnp.where(parity, 0.0, picked)], axis=1
        ).astype(BF16)

    x = x_ref[...].astype(F32)
    centred = x - jnp.mean(x, axis=-1, keepdims=True)
    ready = (
        centred * lax.rsqrt(jnp.mean(centred * centred, axis=-1, keepdims=True) + EPS)
        * in_gain_ref[...]
    ).astype(BF16)
    ready_ref[...] = ready
    for ch in range(2):
        spread_ref[2 * ch] = spread((lw_ref, rw_ref), ch)
        spread_ref[2 * ch + 1] = spread((lg_ref, rg_ref), ch)
    both = jnp.concatenate([ready_ref[:lines, :], ready_ref[lines:, :]], axis=1)

    for ch in range(2):
        value = dot_nt(spread_ref[2 * ch], both) * sigmoid(dot_nt(spread_ref[2 * ch + 1], both))
        send1[ch] = value.reshape(group, 4, lines).astype(BF16)
        if ch == 0:
            pl.semaphore_wait(barrier, len(near))
            for k, (dz, dy, dx) in enumerate(columns):
                signal(known.at[k], [(0, (Y - dy) % Y, (X - dx) % X)])
        send(*leg1(ch), near)
    for k, offset in sorted(enumerate(columns), key=lambda c: everyone.index(c[1]), reverse=True):
        pl.semaphore_wait(known.at[k], 1)
        send(*leg1(0), [o for o in rest if o[1:] == offset[1:]])
    send(*leg1(1), rest)
    for ch in range(2):
        recv1[ch, me] = send1[ch, me]

    gate_ref[...] = sigmoid(
        jnp.dot(ready_ref[...], og_ref[...], preferred_element_type=F32)
    )
    left_ref[...] = jnp.zeros_like(left_ref)
    right_ref[...] = jnp.zeros_like(right_ref)

    per = north // east * 2
    for ch in range(2):
        all_of(*leg1(ch)).wait_recv()
        for s in range(east):
            lines_l = recv1[ch, north * s : north * (s + 1), 0:2, :].reshape(2 * north, lines)
            lines_r = recv1[ch, north * s : north * (s + 1), 2:4, :].reshape(2 * north, lines)
            for i in range(half):
                left_ref[2 * north * i : 2 * north * (i + 1), 128 * s : 128 * s + cols] = (
                    lines_l[:, cols * i : cols * (i + 1)]
                )
                piece = lines_r[:, cols * i : cols * (i + 1)]
                for t in range(east):
                    right_ref[128 * t + per * i : 128 * t + per * (i + 1), 128 * s : 128 * s + cols] = (
                        piece[per * t : per * (t + 1)]
                    )
        mixed = dot_nt(left_ref[...], right_ref[...]) * (cols * east) ** (-0.5)
        for t in range(east):
            strip = jnp.concatenate(
                [
                    mixed[2 * north * i : 2 * north * (i + 1), 128 * t : 128 * t + cols]
                    for i in range(half)
                ],
                axis=1,
            )
            send2[ch, north * t : north * (t + 1)] = strip.reshape(north, 2, lines).astype(BF16)
        for i in range(len(parts)):
            if parts[i][0] == ch:
                send(*leg2(i), everyone)
        recv2[ch, me] = send2[ch, me]

    mid_gain = jnp.broadcast_to(mid_gain_ref[...], (width, width)).T
    mid_gain = jnp.broadcast_to(mid_gain[:, None, :], (width, 2, width)).reshape(2 * width, width)
    mid_gain = jnp.concatenate([mid_gain] * 3, axis=1)
    weight = ow_ref[...].astype(F32)
    weight = jnp.broadcast_to(weight[:, None, :], (width, 2, width)).reshape(2 * width, width)
    first = (iota((2 * width, width), 0) & 1) == 0
    weight = jnp.concatenate(
        [jnp.where(first, weight, 0.0), jnp.where(first, 0.0, weight)], axis=1
    ).astype(BF16)
    lane = iota((tile, tile), 1)
    block = jnp.where(lane >= 2 * cols, 2, 0)
    block = block + jnp.where(lane - block * cols >= cols, 1, 0)
    rest = lane - block * cols
    target = block * cols + ((rest & (per - 1)) >> 1) * rows + (rest & 1) * half + (rest >> 3)
    order = jnp.where(iota((tile, tile), 0) == target, 1.0, 0.0).astype(BF16)

    def fold(total):
        total = jnp.sum(total.reshape(width // 8, 8, lines), axis=0)
        total = total + pltpu.roll(total, 4, 0)
        return (total + pltpu.roll(total, 2, 0)) * (2.0 / width)

    def centre(values, middle):
        return (values.reshape(width // 8, 8, lines) - middle[None]).reshape(width, lines)

    all_of(*leg2(0)).wait_recv()
    mixed = recv2[0].reshape(width, lines).astype(F32)
    mean0 = fold(mixed)
    mixed = centre(mixed, mean0)
    mixed_ref[...] = mixed
    mean_ref[...] = mean0
    spread0_ref[...] = fold(mixed * mixed)
    all_of(*leg2(1)).wait_recv()
    mixed = recv2[1].reshape(width, lines).astype(F32)
    mean1 = fold(mixed)
    mixed = centre(mixed, mean1)
    step = 0.5 * (mean1 - mean_ref[...])
    variance = 0.5 * (fold(mixed * mixed) + spread0_ref[...]) + step * step
    scale = lax.rsqrt(variance + EPS)

    for g in range(lines // tile):
        lanes = slice(g * tile, (g + 1) * tile)

        def finish(values, shift, gain):
            values = values.reshape(width // 8, 8, tile) + shift[None, :, lanes]
            return ((values * scale[None, :, lanes]).reshape(width, tile) * gain).astype(BF16)

        scaled = jnp.concatenate(
            [
                finish(mixed_ref[:, lanes], -step, mid_gain[:width]),
                finish(mixed[:, lanes], step, mid_gain[width:]),
            ],
            axis=0,
        )
        turned = dot_nt(order, scaled).astype(BF16)
        result = jnp.dot(turned, weight, preferred_element_type=F32)
        for h in range(2):
            at = slice(h * lines + g * tile, h * lines + (g + 1) * tile)
            out_ref[at, :] = (
                result[:, h * width : (h + 1) * width] * gate_ref[at, :]
            ).astype(BF16)

    for ch in range(2):
        all_of(*leg1(ch)).wait_send()
    for i in range(len(parts)):
        all_of(*leg2(i)).wait_send()


def local(
    north,
    east,
    pair_state,
    in_gain,
    left_weight,
    right_weight,
    left_gate,
    right_gate,
    mid_gain,
    out_weight,
    out_gate,
):
    rows, cols, width = pair_state.shape
    lines = rows // 2 * cols
    group = north * east
    vmem = pl.BlockSpec(memory_space=pltpu.VMEM)
    out = pl.pallas_call(
        functools.partial(kernel, north, east, rows, cols),
        out_shape=pltpu.VMEM((rows * cols, width), BF16),
        in_specs=[pl.BlockSpec(memory_space=pltpu.HBM)] * 9,
        out_specs=vmem,
        scratch_shapes=[
            pltpu.VMEM((rows * cols, width), BF16),
            pltpu.VMEM((1, width), F32),
            pltpu.VMEM((width, width), BF16),
            pltpu.VMEM((width, width), BF16),
            pltpu.VMEM((width, width), BF16),
            pltpu.VMEM((width, width), BF16),
            pltpu.VMEM((1, width), F32),
            pltpu.VMEM((width, width), BF16),
            pltpu.VMEM((width, width), BF16),
            pltpu.SemaphoreType.DMA((9,)),
            pltpu.VMEM((rows * cols, width), BF16),
            pltpu.VMEM((rows * cols, width), F32),
            pltpu.VMEM((2, group, 4, lines), BF16),
            pltpu.VMEM((2, group, 4, lines), BF16),
            pltpu.VMEM((rows * north, 128 * east), BF16),
            pltpu.VMEM((128 * east, 128 * east), BF16),
            pltpu.VMEM((2, group, 2, lines), BF16),
            pltpu.VMEM((2, group, 2, lines), BF16),
            pltpu.SemaphoreType.DMA((2,)),
            pltpu.SemaphoreType.DMA((2,)),
            pltpu.SemaphoreType.DMA((2,)),
            pltpu.SemaphoreType.DMA((2,)),
            pltpu.SemaphoreType.REGULAR((Y * X - 1,)),
            pltpu.VMEM((4, 4 * group, 2 * width), BF16),
            pltpu.VMEM((width, lines), F32),
            pltpu.VMEM((8, lines), F32),
            pltpu.VMEM((8, lines), F32),
        ],
        compiler_params=pltpu.CompilerParams(
            collective_id=0, has_side_effects=True, vmem_limit_bytes=48 * 1024 * 1024
        ),
    )(
        *(
            pltpu.with_memory_space_constraint(a, pltpu.HBM)
            for a in (
                pair_state.reshape(rows * cols, width),
                in_gain.reshape(1, width),
                left_weight,
                right_weight,
                left_gate,
                right_gate,
                mid_gain.reshape(1, width),
                out_weight,
                out_gate,
            )
        )
    )
    return out.reshape(rows, cols, width)


def solution(mesh):
    north, east = mesh.shape["north"], mesh.shape["east"]
    return jax.shard_map(
        functools.partial(local, north, east),
        mesh=mesh,
        in_specs=(
            P(("trial", "north"), "east", None),
            P(),
            P("trial", None),
            P("trial", None),
            P("trial", None),
            P("trial", None),
            P(),
            P("trial", None),
            P("trial", None),
        ),
        out_specs=P(("trial", "north"), "east", None),
        check_vma=False,
    )
```

```python
import functools

import jax
import jax.numpy as jnp
from jax import lax
from jax.experimental import pallas as pl
from jax.experimental.pallas import tpu as pltpu
from jax.sharding import PartitionSpec as P

MESH = pl.DeviceIdType.MESH
BF16, F32 = jnp.bfloat16, jnp.float32
Y, X = 4, 2
EPS = 1e-05


def dot_nt(a, b):
    return lax.dot_general(a, b, (((1,), (1,)), ((), ())), preferred_element_type=F32)


def iota(shape, axis):
    return lax.broadcasted_iota(jnp.int32, shape, axis)


def sigmoid(x):
    return jax.nn.sigmoid(x)


def kernel(
    north,
    east,
    rows,
    cols,
    x_hbm,
    in_gain_hbm,
    lw_hbm,
    rw_hbm,
    lg_hbm,
    rg_hbm,
    mid_gain_hbm,
    ow_hbm,
    og_hbm,
    out_ref,
    x_ref,
    in_gain_ref,
    lw_ref,
    rw_ref,
    lg_ref,
    rg_ref,
    mid_gain_ref,
    ow_ref,
    og_ref,
    load_sem,
    ready_ref,
    gate_ref,
    send1,
    recv1,
    left_ref,
    right_ref,
    send2,
    recv2,
    send_sem1,
    recv_sem1,
    send_sem2,
    recv_sem2,
    known,
    spread_ref,
    mixed_ref,
    mean_ref,
    spread0_ref,
    strip_ref,
):
    loads = [
        pltpu.make_async_copy(src, dst, load_sem.at[i])
        for i, (src, dst) in enumerate(
            (
                (x_hbm, x_ref),
                (in_gain_hbm, in_gain_ref),
                (lw_hbm, lw_ref),
                (rw_hbm, rw_ref),
                (lg_hbm, lg_ref),
                (rg_hbm, rg_ref),
                (mid_gain_hbm, mid_gain_ref),
                (ow_hbm, ow_ref),
                (og_hbm, og_ref),
            )
        )
    ]
    for load in loads:
        load.start()
    width = x_ref.shape[1]
    group = north * east
    half = rows // 2
    lines = half * cols
    n = lax.axis_index("north")
    e = lax.axis_index("east")
    me = e * north + n

    at_z, at_y, at_x = n // (Y * X) * east + e, lax.rem(n // X, Y), lax.rem(n, X)
    depth = group // (Y * X)
    everyone = [(a, b, c) for a in range(depth) for b in range(Y) for c in range(X)][1:]
    everyone.sort(key=lambda o: -min(o[0], depth - o[0]) - min(o[1], Y - o[1]) - 2 * o[2])
    columns = [o for o in everyone if o[0] == 0]
    near = [o for o in everyone if o in columns or o[1:] == (0, 0)]
    rest = [o for o in everyone if o not in near]

    def each_peer(offsets, do):
        for dz, dy, dx in offsets:
            pz = lax.rem(at_z + dz, depth)
            north_of = (pz // east * Y + lax.rem(at_y + dy, Y)) * X + lax.rem(at_x + dx, X)
            east_of = lax.rem(pz, east)
            do(east_of * north + north_of, {"north": north_of, "east": east_of})

    def signal(semaphore, offsets):
        each_peer(
            offsets,
            lambda q, device: pl.semaphore_signal(
                semaphore, inc=1, device_id=device, device_id_type=MESH
            ),
        )

    barrier = pltpu.get_barrier_semaphore()
    signal(barrier, near)

    def send(src, dst, send_sem, recv_sem, offsets):
        each_peer(
            offsets,
            lambda q, device: pltpu.make_async_remote_copy(
                src_ref=src(q),
                dst_ref=dst(me),
                send_sem=send_sem,
                recv_sem=recv_sem,
                device_id=device,
                device_id_type=MESH,
            ).start(),
        )

    def all_of(src, dst, send_sem, recv_sem):
        most = pl.ds(0, group - 1)
        return pltpu.make_async_remote_copy(
            src_ref=src(most),
            dst_ref=dst(most),
            send_sem=send_sem,
            recv_sem=recv_sem,
            device_id={"north": n, "east": e},
            device_id_type=MESH,
        )

    def leg1(ch):
        return (
            lambda q: send1.at[ch, q],
            lambda q: recv1.at[ch, q],
            send_sem1.at[ch],
            recv_sem1.at[ch],
        )

    tile = 4 * cols
    parts = ((0, 0, 3), (1, 0, 3))

    def leg2(i):
        ch, start, stop = parts[i]
        lanes = pl.ds(start * tile, (stop - start) * tile)
        return (
            lambda q: send2.at[ch, q, :, lanes],
            lambda q: recv2.at[ch, q, :, lanes],
            send_sem2.at[i],
            recv_sem2.at[i],
        )

    for load in loads:
        load.wait()
    r = iota((4 * group, width), 0)
    d = iota((4 * group, width), 1)
    parity = (r & 1) == 0

    def spread(weights, ch):
        picked = 0.0
        for f, w in enumerate(weights):
            pick = (((r >> 1) & 1) == f) & (d == (r >> 2) + ch * group)
            picked = picked + dot_nt(jnp.where(pick, 1.0, 0.0).astype(BF16), w[...])
        return jnp.concatenate(
            [jnp.where(parity, picked, 0.0), jnp.where(parity, 0.0, picked)], axis=1
        ).astype(BF16)

    for c in range(0, 2 * lines, 128):
        some = slice(c, c + 128)
        x = x_ref[some, :].astype(F32)
        centred = x - jnp.mean(x, axis=-1, keepdims=True)
        ready_ref[some, :] = (
            centred
            * lax.rsqrt(jnp.mean(centred * centred, axis=-1, keepdims=True) + EPS)
            * in_gain_ref[...]
        ).astype(BF16)
    for ch in range(2):
        spread_ref[2 * ch] = spread((lw_ref, rw_ref), ch)
        spread_ref[2 * ch + 1] = spread((lg_ref, rg_ref), ch)
    both = jnp.concatenate([ready_ref[:lines, :], ready_ref[lines:, :]], axis=1)

    for ch in range(2):
        for g in range(0, lines, tile):
            some = both[g : g + tile, :]
            value = dot_nt(spread_ref[2 * ch], some) * sigmoid(dot_nt(spread_ref[2 * ch + 1], some))
            send1[ch, :, :, g : g + tile] = value.reshape(group, 4, tile).astype(BF16)
        if ch == 0:
            pl.semaphore_wait(barrier, len(near))
            for k, (dz, dy, dx) in enumerate(columns):
                signal(known.at[k], [(0, (Y - dy) % Y, (X - dx) % X)])

        @pl.when(at_z >= 0)
        def _(ch=ch):
            send(*leg1(ch), near)

    for k, offset in sorted(enumerate(columns), key=lambda c: everyone.index(c[1]), reverse=True):
        pl.semaphore_wait(known.at[k], 1)
        send(*leg1(0), [o for o in rest if o[1:] == offset[1:]])
    send(*leg1(1), rest)
    for ch in range(2):
        recv1[ch, me] = send1[ch, me]

    gate_ref[...] = sigmoid(
        jnp.dot(ready_ref[...], og_ref[...], preferred_element_type=F32)
    )
    left_ref[...] = jnp.zeros_like(left_ref)
    right_ref[...] = jnp.zeros_like(right_ref)

    per = north // east * 2
    lane = iota((tile, tile), 1)
    block = jnp.where(lane >= 2 * cols, 2, 0)
    block = block + jnp.where(lane - block * cols >= cols, 1, 0)
    rest = lane - block * cols
    target = block * cols + ((rest & (per - 1)) >> 1) * rows + (rest & 1) * half + (rest >> 3)
    order = jnp.where(iota((tile, tile), 0) == target, 1.0, 0.0).astype(BF16)

    for ch in range(2):
        all_of(*leg1(ch)).wait_recv()
        for s in range(east):
            lines_l = recv1[ch, north * s : north * (s + 1), 0:2, :].reshape(2 * north, lines)
            lines_r = recv1[ch, north * s : north * (s + 1), 2:4, :].reshape(2 * north, lines)
            for i in range(half):
                left_ref[2 * north * i : 2 * north * (i + 1), 128 * s : 128 * s + cols] = (
                    lines_l[:, cols * i : cols * (i + 1)]
                )
                piece = lines_r[:, cols * i : cols * (i + 1)]
                for t in range(east):
                    right_ref[128 * t + per * i : 128 * t + per * (i + 1), 128 * s : 128 * s + cols] = (
                        piece[per * t : per * (t + 1)]
                    )
        mixed = dot_nt(left_ref[...], right_ref[...]) * (cols * east) ** (-0.5)
        for t in range(east):
            strip = jnp.concatenate(
                [
                    mixed[2 * north * i : 2 * north * (i + 1), 128 * t : 128 * t + cols]
                    for i in range(half)
                ],
                axis=1,
            )
            strip_ref[2 * north * t : 2 * north * (t + 1), :] = strip.astype(BF16)
        for g in range(lines // tile):
            lanes = slice(g * tile, (g + 1) * tile)
            strip = dot_nt(strip_ref[:, lanes], order)
            send2[ch, :, :, lanes] = strip.reshape(group, 2, tile).astype(BF16)
        for i in range(len(parts)):
            if parts[i][0] == ch:
                send(*leg2(i), everyone)
        recv2[ch, me] = send2[ch, me]

    mid_gain = jnp.broadcast_to(mid_gain_ref[...], (width, width)).T
    mid_gain = jnp.broadcast_to(mid_gain[:, None, :], (width, 2, width)).reshape(2 * width, width)
    mid_gain = jnp.concatenate([mid_gain] * 3, axis=1)
    weight = ow_ref[...].astype(F32)
    weight = jnp.broadcast_to(weight[:, None, :], (width, 2, width)).reshape(2 * width, width)
    first = (iota((2 * width, width), 0) & 1) == 0
    weight = jnp.concatenate(
        [jnp.where(first, weight, 0.0), jnp.where(first, 0.0, weight)], axis=1
    ).astype(BF16)
    def fold(total):
        total = jnp.sum(total, axis=0)
        total = total + pltpu.roll(total, 4, 0)
        return (total + pltpu.roll(total, 2, 0)) * (2.0 / width)

    def take(ch, lanes):
        values = recv2[ch, :, :, lanes].reshape(width, tile).astype(F32)
        values = values.reshape(width // 8, 8, tile)
        mean = fold(values)
        values = values - mean[None]
        return values, mean, fold(values * values)

    tiles = [slice(g * tile, (g + 1) * tile) for g in range(lines // tile)]
    all_of(*leg2(0)).wait_recv()
    for lanes in tiles:
        values, mean_ref[:, lanes], spread0_ref[:, lanes] = take(0, lanes)
        mixed_ref[:, lanes] = values.reshape(width, tile)
    all_of(*leg2(1)).wait_recv()
    for g, lanes in enumerate(tiles):
        values, mean, variance = take(1, lanes)
        step = 0.5 * (mean - mean_ref[:, lanes])
        variance = 0.5 * (variance + spread0_ref[:, lanes]) + step * step
        scale = lax.rsqrt(variance + EPS)

        def finish(values, shift, gain):
            values = (values + shift[None]) * scale[None]
            return (values.reshape(width, tile) * gain).astype(BF16)

        scaled = jnp.concatenate(
            [
                finish(
                    mixed_ref[:, lanes].reshape(width // 8, 8, tile), -step, mid_gain[:width]
                ),
                finish(values, step, mid_gain[width:]),
            ],
            axis=0,
        )
        result = lax.dot_general(
            scaled, weight, (((0,), (0,)), ((), ())), preferred_element_type=F32
        )
        for h in range(2):
            at = slice(h * lines + g * tile, h * lines + (g + 1) * tile)
            out_ref[at, :] = (
                result[:, h * width : (h + 1) * width] * gate_ref[at, :]
            ).astype(BF16)

    for ch in range(2):
        all_of(*leg1(ch)).wait_send()
    for i in range(len(parts)):
        all_of(*leg2(i)).wait_send()


def local(
    north,
    east,
    pair_state,
    in_gain,
    left_weight,
    right_weight,
    left_gate,
    right_gate,
    mid_gain,
    out_weight,
    out_gate,
):
    rows, cols, width = pair_state.shape
    lines = rows // 2 * cols
    group = north * east
    vmem = pl.BlockSpec(memory_space=pltpu.VMEM)
    out = pl.pallas_call(
        functools.partial(kernel, north, east, rows, cols),
        out_shape=pltpu.VMEM((rows * cols, width), BF16),
        in_specs=[pl.BlockSpec(memory_space=pltpu.HBM)] * 9,
        out_specs=vmem,
        scratch_shapes=[
            pltpu.VMEM((rows * cols, width), BF16),
            pltpu.VMEM((1, width), F32),
            pltpu.VMEM((width, width), BF16),
            pltpu.VMEM((width, width), BF16),
            pltpu.VMEM((width, width), BF16),
            pltpu.VMEM((width, width), BF16),
            pltpu.VMEM((1, width), F32),
            pltpu.VMEM((width, width), BF16),
            pltpu.VMEM((width, width), BF16),
            pltpu.SemaphoreType.DMA((9,)),
            pltpu.VMEM((rows * cols, width), BF16),
            pltpu.VMEM((rows * cols, width), F32),
            pltpu.VMEM((2, group, 4, lines), BF16),
            pltpu.VMEM((2, group, 4, lines), BF16),
            pltpu.VMEM((rows * north, 128 * east), BF16),
            pltpu.VMEM((128 * east, 128 * east), BF16),
            pltpu.VMEM((2, group, 2, lines), BF16),
            pltpu.VMEM((2, group, 2, lines), BF16),
            pltpu.SemaphoreType.DMA((2,)),
            pltpu.SemaphoreType.DMA((2,)),
            pltpu.SemaphoreType.DMA((2,)),
            pltpu.SemaphoreType.DMA((2,)),
            pltpu.SemaphoreType.REGULAR((Y * X - 1,)),
            pltpu.VMEM((4, 4 * group, 2 * width), BF16),
            pltpu.VMEM((width, lines), F32),
            pltpu.VMEM((8, lines), F32),
            pltpu.VMEM((8, lines), F32),
            pltpu.VMEM((2 * group, lines), BF16),
        ],
        compiler_params=pltpu.CompilerParams(
            collective_id=0, has_side_effects=True, vmem_limit_bytes=48 * 1024 * 1024
        ),
    )(
        *(
            pltpu.with_memory_space_constraint(a, pltpu.HBM)
            for a in (
                pair_state.reshape(rows * cols, width),
                in_gain.reshape(1, width),
                left_weight,
                right_weight,
                left_gate,
                right_gate,
                mid_gain.reshape(1, width),
                out_weight,
                out_gate,
            )
        )
    )
    return out.reshape(rows, cols, width)


def solution(mesh):
    north, east = mesh.shape["north"], mesh.shape["east"]
    return jax.shard_map(
        functools.partial(local, north, east),
        mesh=mesh,
        in_specs=(
            P(("trial", "north"), "east", None),
            P(),
            P("trial", None),
            P("trial", None),
            P("trial", None),
            P("trial", None),
            P(),
            P("trial", None),
            P("trial", None),
        ),
        out_specs=P(("trial", "north"), "east", None),
        check_vma=False,
    )
```

```python
import functools

import jax
import jax.numpy as jnp
from jax import lax
from jax.experimental import pallas as pl
from jax.experimental.pallas import tpu as pltpu
from jax.sharding import PartitionSpec as P

MESH = pl.DeviceIdType.MESH
BF16, F32 = jnp.bfloat16, jnp.float32
Y, X = 4, 2
EPS = 1e-05


def dot_nt(a, b):
    return lax.dot_general(a, b, (((1,), (1,)), ((), ())), preferred_element_type=F32)


def iota(shape, axis):
    return lax.broadcasted_iota(jnp.int32, shape, axis)


def sigmoid(x):
    return jax.nn.sigmoid(x)


def kernel(
    north,
    east,
    rows,
    cols,
    x_hbm,
    in_gain_hbm,
    lw_hbm,
    rw_hbm,
    lg_hbm,
    rg_hbm,
    mid_gain_hbm,
    ow_hbm,
    og_hbm,
    out_ref,
    x_ref,
    in_gain_ref,
    lw_ref,
    rw_ref,
    lg_ref,
    rg_ref,
    mid_gain_ref,
    ow_ref,
    og_ref,
    load_sem,
    ready_ref,
    gate_ref,
    send1,
    recv1,
    left_ref,
    right_ref,
    send2,
    recv2,
    send_sem1,
    recv_sem1,
    send_sem2,
    recv_sem2,
    known,
    spread_ref,
    mixed_ref,
    mean_ref,
    spread0_ref,
    strip_ref,
):
    loads = [
        pltpu.make_async_copy(src, dst, load_sem.at[i])
        for i, (src, dst) in enumerate(
            (
                (x_hbm, x_ref),
                (in_gain_hbm, in_gain_ref),
                (lw_hbm, lw_ref),
                (rw_hbm, rw_ref),
                (lg_hbm, lg_ref),
                (rg_hbm, rg_ref),
                (mid_gain_hbm, mid_gain_ref),
                (ow_hbm, ow_ref),
                (og_hbm, og_ref),
            )
        )
    ]
    for load in loads:
        load.start()
    width = x_ref.shape[1]
    group = north * east
    half = rows // 2
    lines = half * cols
    n = lax.axis_index("north")
    e = lax.axis_index("east")
    me = e * north + n

    at_z, at_y, at_x = n // (Y * X) * east + e, lax.rem(n // X, Y), lax.rem(n, X)
    depth = group // (Y * X)
    everyone = [(a, b, c) for a in range(depth) for b in range(Y) for c in range(X)][1:]
    everyone.sort(key=lambda o: -min(o[0], depth - o[0]) - min(o[1], Y - o[1]) - 2 * o[2])
    columns = [o for o in everyone if o[0] == 0]
    near = [o for o in everyone if o in columns or o[1:] == (0, 0)]
    rest = [o for o in everyone if o not in near]

    def each_peer(offsets, do):
        for dz, dy, dx in offsets:
            pz = lax.rem(at_z + dz, depth)
            north_of = (pz // east * Y + lax.rem(at_y + dy, Y)) * X + lax.rem(at_x + dx, X)
            east_of = lax.rem(pz, east)
            do(east_of * north + north_of, {"north": north_of, "east": east_of})

    def signal(semaphore, offsets):
        each_peer(
            offsets,
            lambda q, device: pl.semaphore_signal(
                semaphore, inc=1, device_id=device, device_id_type=MESH
            ),
        )

    barrier = pltpu.get_barrier_semaphore()
    signal(barrier, near)

    def send(src, dst, send_sem, recv_sem, offsets):
        each_peer(
            offsets,
            lambda q, device: pltpu.make_async_remote_copy(
                src_ref=src(q),
                dst_ref=dst(me),
                send_sem=send_sem,
                recv_sem=recv_sem,
                device_id=device,
                device_id_type=MESH,
            ).start(),
        )

    def all_of(src, dst, send_sem, recv_sem):
        most = pl.ds(0, group - 1)
        return pltpu.make_async_remote_copy(
            src_ref=src(most),
            dst_ref=dst(most),
            send_sem=send_sem,
            recv_sem=recv_sem,
            device_id={"north": n, "east": e},
            device_id_type=MESH,
        )

    def leg1(ch):
        return (
            lambda q: send1.at[ch, q],
            lambda q: recv1.at[ch, q],
            send_sem1.at[ch],
            recv_sem1.at[ch],
        )

    tile = 4 * cols
    parts = ((0, 0, 3), (1, 0, 3))

    def leg2(i):
        ch, start, stop = parts[i]
        lanes = pl.ds(start * tile, (stop - start) * tile)
        return (
            lambda q: send2.at[ch, q, :, lanes],
            lambda q: recv2.at[ch, q, :, lanes],
            send_sem2.at[i],
            recv_sem2.at[i],
        )

    for load in loads:
        load.wait()
    r = iota((4 * group, width), 0)
    d = iota((4 * group, width), 1)
    parity = (r & 1) == 0

    def spread(weights, ch):
        picked = 0.0
        for f, w in enumerate(weights):
            pick = (((r >> 1) & 1) == f) & (d == (r >> 2) + ch * group)
            picked = picked + dot_nt(jnp.where(pick, 1.0, 0.0).astype(BF16), w[...])
        return jnp.concatenate(
            [jnp.where(parity, picked, 0.0), jnp.where(parity, 0.0, picked)], axis=1
        ).astype(BF16)

    for c in range(0, 2 * lines, 128):
        some = slice(c, c + 128)
        x = x_ref[some, :].astype(F32)
        centred = x - jnp.mean(x, axis=-1, keepdims=True)
        ready_ref[some, :] = (
            centred
            * lax.rsqrt(jnp.mean(centred * centred, axis=-1, keepdims=True) + EPS)
            * in_gain_ref[...]
        ).astype(BF16)
    for ch in range(2):
        spread_ref[2 * ch] = spread((lw_ref, rw_ref), ch)
        spread_ref[2 * ch + 1] = spread((lg_ref, rg_ref), ch)
    both = jnp.concatenate([ready_ref[:lines, :], ready_ref[lines:, :]], axis=1)

    for ch in range(2):
        for g in range(0, lines, tile):
            some = both[g : g + tile, :]
            value = dot_nt(spread_ref[2 * ch], some) * sigmoid(dot_nt(spread_ref[2 * ch + 1], some))
            send1[ch, :, :, g : g + tile] = value.reshape(group, 4, tile).astype(BF16)
    pl.semaphore_wait(barrier, len(near))
    for k, (dz, dy, dx) in enumerate(columns):
        signal(known.at[k], [(0, (Y - dy) % Y, (X - dx) % X)])
    send(*leg1(0), near)
    send(*leg1(1), near)
    for k, offset in sorted(enumerate(columns), key=lambda c: everyone.index(c[1]), reverse=True):
        pl.semaphore_wait(known.at[k], 1)
        send(*leg1(0), [o for o in rest if o[1:] == offset[1:]])
    send(*leg1(1), rest)
    for ch in range(2):
        recv1[ch, me] = send1[ch, me]

    gate_ref[...] = sigmoid(
        jnp.dot(ready_ref[...], og_ref[...], preferred_element_type=F32)
    )
    left_ref[...] = jnp.zeros_like(left_ref)
    right_ref[...] = jnp.zeros_like(right_ref)

    per = north // east * 2
    lane = iota((tile, tile), 1)
    block = jnp.where(lane >= 2 * cols, 2, 0)
    block = block + jnp.where(lane - block * cols >= cols, 1, 0)
    rest = lane - block * cols
    target = block * cols + ((rest & (per - 1)) >> 1) * rows + (rest & 1) * half + (rest >> 3)
    order = jnp.where(iota((tile, tile), 0) == target, 1.0, 0.0).astype(BF16)

    for ch in range(2):
        all_of(*leg1(ch)).wait_recv()
        for s in range(east):
            lines_l = recv1[ch, north * s : north * (s + 1), 0:2, :].reshape(2 * north, lines)
            lines_r = recv1[ch, north * s : north * (s + 1), 2:4, :].reshape(2 * north, lines)
            for i in range(half):
                left_ref[2 * north * i : 2 * north * (i + 1), 128 * s : 128 * s + cols] = (
                    lines_l[:, cols * i : cols * (i + 1)]
                )
                piece = lines_r[:, cols * i : cols * (i + 1)]
                for t in range(east):
                    right_ref[128 * t + per * i : 128 * t + per * (i + 1), 128 * s : 128 * s + cols] = (
                        piece[per * t : per * (t + 1)]
                    )
        mixed = dot_nt(left_ref[...], right_ref[...]) * (cols * east) ** (-0.5)
        for t in range(east):
            strip = jnp.concatenate(
                [
                    mixed[2 * north * i : 2 * north * (i + 1), 128 * t : 128 * t + cols]
                    for i in range(half)
                ],
                axis=1,
            )
            strip_ref[2 * north * t : 2 * north * (t + 1), :] = strip.astype(BF16)
        for g in range(lines // tile):
            lanes = slice(g * tile, (g + 1) * tile)
            strip = dot_nt(strip_ref[:, lanes], order)
            send2[ch, :, :, lanes] = strip.reshape(group, 2, tile).astype(BF16)
        for i in range(len(parts)):
            if parts[i][0] == ch:
                send(*leg2(i), everyone)
        recv2[ch, me] = send2[ch, me]

    mid_gain = jnp.broadcast_to(mid_gain_ref[...], (width, width)).T
    mid_gain = jnp.broadcast_to(mid_gain[:, None, :], (width, 2, width)).reshape(2 * width, width)
    mid_gain = jnp.concatenate([mid_gain] * 3, axis=1)
    weight = ow_ref[...].astype(F32)
    weight = jnp.broadcast_to(weight[:, None, :], (width, 2, width)).reshape(2 * width, width)
    first = (iota((2 * width, width), 0) & 1) == 0
    weight = jnp.concatenate(
        [jnp.where(first, weight, 0.0), jnp.where(first, 0.0, weight)], axis=1
    ).astype(BF16)
    def fold(total):
        total = jnp.sum(total, axis=0)
        total = total + pltpu.roll(total, 4, 0)
        return (total + pltpu.roll(total, 2, 0)) * (2.0 / width)

    def take(ch, lanes):
        values = recv2[ch, :, :, lanes].reshape(width, tile).astype(F32)
        values = values.reshape(width // 8, 8, tile)
        mean = fold(values)
        values = values - mean[None]
        return values, mean, fold(values * values)

    tiles = [slice(g * tile, (g + 1) * tile) for g in range(lines // tile)]
    all_of(*leg2(0)).wait_recv()
    for lanes in tiles:
        values, mean_ref[:, lanes], spread0_ref[:, lanes] = take(0, lanes)
        mixed_ref[:, lanes] = values.reshape(width, tile)
    all_of(*leg2(1)).wait_recv()
    for g, lanes in enumerate(tiles):
        values, mean, variance = take(1, lanes)
        step = 0.5 * (mean - mean_ref[:, lanes])
        variance = 0.5 * (variance + spread0_ref[:, lanes]) + step * step
        scale = lax.rsqrt(variance + EPS)

        def finish(values, shift, gain):
            values = (values + shift[None]) * scale[None]
            return (values.reshape(width, tile) * gain).astype(BF16)

        scaled = jnp.concatenate(
            [
                finish(
                    mixed_ref[:, lanes].reshape(width // 8, 8, tile), -step, mid_gain[:width]
                ),
                finish(values, step, mid_gain[width:]),
            ],
            axis=0,
        )
        result = lax.dot_general(
            scaled, weight, (((0,), (0,)), ((), ())), preferred_element_type=F32
        )
        for h in range(2):
            at = slice(h * lines + g * tile, h * lines + (g + 1) * tile)
            out_ref[at, :] = (
                result[:, h * width : (h + 1) * width] * gate_ref[at, :]
            ).astype(BF16)

    for ch in range(2):
        all_of(*leg1(ch)).wait_send()
    for i in range(len(parts)):
        all_of(*leg2(i)).wait_send()


def local(
    north,
    east,
    pair_state,
    in_gain,
    left_weight,
    right_weight,
    left_gate,
    right_gate,
    mid_gain,
    out_weight,
    out_gate,
):
    rows, cols, width = pair_state.shape
    lines = rows // 2 * cols
    group = north * east
    vmem = pl.BlockSpec(memory_space=pltpu.VMEM)
    out = pl.pallas_call(
        functools.partial(kernel, north, east, rows, cols),
        out_shape=pltpu.VMEM((rows * cols, width), BF16),
        in_specs=[pl.BlockSpec(memory_space=pltpu.HBM)] * 9,
        out_specs=vmem,
        scratch_shapes=[
            pltpu.VMEM((rows * cols, width), BF16),
            pltpu.VMEM((1, width), F32),
            pltpu.VMEM((width, width), BF16),
            pltpu.VMEM((width, width), BF16),
            pltpu.VMEM((width, width), BF16),
            pltpu.VMEM((width, width), BF16),
            pltpu.VMEM((1, width), F32),
            pltpu.VMEM((width, width), BF16),
            pltpu.VMEM((width, width), BF16),
            pltpu.SemaphoreType.DMA((9,)),
            pltpu.VMEM((rows * cols, width), BF16),
            pltpu.VMEM((rows * cols, width), F32),
            pltpu.VMEM((2, group, 4, lines), BF16),
            pltpu.VMEM((2, group, 4, lines), BF16),
            pltpu.VMEM((rows * north, 128 * east), BF16),
            pltpu.VMEM((128 * east, 128 * east), BF16),
            pltpu.VMEM((2, group, 2, lines), BF16),
            pltpu.VMEM((2, group, 2, lines), BF16),
            pltpu.SemaphoreType.DMA((2,)),
            pltpu.SemaphoreType.DMA((2,)),
            pltpu.SemaphoreType.DMA((2,)),
            pltpu.SemaphoreType.DMA((2,)),
            pltpu.SemaphoreType.REGULAR((Y * X - 1,)),
            pltpu.VMEM((4, 4 * group, 2 * width), BF16),
            pltpu.VMEM((width, lines), F32),
            pltpu.VMEM((8, lines), F32),
            pltpu.VMEM((8, lines), F32),
            pltpu.VMEM((2 * group, lines), BF16),
        ],
        compiler_params=pltpu.CompilerParams(
            collective_id=0, has_side_effects=True, vmem_limit_bytes=48 * 1024 * 1024
        ),
    )(
        *(
            pltpu.with_memory_space_constraint(a, pltpu.HBM)
            for a in (
                pair_state.reshape(rows * cols, width),
                in_gain.reshape(1, width),
                left_weight,
                right_weight,
                left_gate,
                right_gate,
                mid_gain.reshape(1, width),
                out_weight,
                out_gate,
            )
        )
    )
    return out.reshape(rows, cols, width)


def solution(mesh):
    north, east = mesh.shape["north"], mesh.shape["east"]
    return jax.shard_map(
        functools.partial(local, north, east),
        mesh=mesh,
        in_specs=(
            P(("trial", "north"), "east", None),
            P(),
            P("trial", None),
            P("trial", None),
            P("trial", None),
            P("trial", None),
            P(),
            P("trial", None),
            P("trial", None),
        ),
        out_specs=P(("trial", "north"), "east", None),
        check_vma=False,
    )
```
